512 devices in a mesh: section: 8 (over z_hi, core), dp: 64 (over y, x, z_lo).
Axes of the slice: x: 4, y: 8, z: 8 (z_hi: 4, z_lo: 2; z = z_hi * 2 + z_lo), core: 2. Of those that a mesh axis runs over, the one named last changes fastest.
Arguments:
- tokens: bfloat16 [2, 64, 80, 1024], P(None, 'dp'), may hold values from -6 to 6
- w_qkv: bfloat16 [8, 1024, 1536], P('section', 'dp'), may hold values from -0.1875 to 0.1875
- w_output: bfloat16 [8, 512, 1024], P('section', None, 'dp'), may hold values from -0.25 to 0.25
- tangent_value: bfloat16 [8, 2, 1024, 512], P('section', None, 'dp'), may hold values from -0.1875 to 0.1875
- tangent_output: bfloat16 [8, 2, 512, 1024], P('section', None, None, 'dp'), may hold values from -0.25 to 0.25
- layer_gain: float32 [8, 1024], P('section'), may hold values from 0.5 to 1.5
- final_gain: float32 [1024], replicated, may hold values from 0.5 to 1.5
- head: bfloat16 [1024, 1000], P(None, 'section'), may hold values from -0.1875 to 0.1875
Outputs:
- mean_logits: float32 [2, 64, 1000], P(None, 'dp', 'section')
- variance: float32 [2, 64, 1000], P(None, 'dp', 'section')
The draws below stay inside these ranges and needn't reach their ends.
All inputs are finite; a program needn't handle non-finite values.
Results may differ from the reference program's by a relative error of at most 0.018.
Values may be sent and summed in bfloat16 or wider, within the bound.
No kernel may reach another device: no remote copies, remote signals or barrier semaphores. Data moves between devices by JAX's collectives and lax.ppermute only.
A program may use at most 64 MiB of HBM per device.

```python
import jax
import jax.numpy as jnp
from jax import lax

D = 1024
HEADS = 8
HEAD = 64
CLASSES = 1000
TOK = 80
TANGENTS = 2
MICRO = 2
HD = 512
IMAGES = 64
SECTIONS = 8
N_SECTION = 8


def level_of(rng, extent, cuts, least, largest):
    def one(dim, shards_of):
        draws = jax.random.uniform(jax.random.fold_in(jax.random.fold_in(rng, 6), dim), (shards_of,), jnp.float32, least / len(cuts), largest / len(cuts))
        return jnp.repeat(jnp.exp(draws), extent[dim] // shards_of).reshape((-1,) + (1,) * (len(extent) - dim - 1))

    factor_of = one(*cuts[0])
    for cut in cuts[1:]:
        factor_of = factor_of * one(*cut)
    return factor_of


def bell_draw(stream_key, extent, spread, reach, split=(), held_as=jnp.bfloat16):
    result = jax.random.normal(stream_key, extent, jnp.float32) * spread
    if len(split) > 0:
        result = level_of(stream_key, extent, split, -0.22, 0.18) * result
    return jnp.clip(result, min=-reach, max=reach).astype(held_as)


def setup_inputs(seed: int = 0) -> dict:
    key_of = jax.random.split(jax.random.key(seed), 9)
    tokens = bell_draw(key_of[0], (MICRO, IMAGES, TOK, D), 1.0, 6.0, ((1, 64),))
    w_qkv = bell_draw(key_of[1], (SECTIONS, D, 3 * HD), D ** -0.5, 0.1875, ((0, 8), (1, 64)))
    w_output = bell_draw(key_of[2], (SECTIONS, HD, D), HD ** -0.5, 0.25, ((0, 8), (2, 64)))
    tangent_value = bell_draw(key_of[3], (SECTIONS, TANGENTS, D, HD), D ** -0.5, 0.1875, ((0, 8), (2, 64)))
    tangent_output = bell_draw(key_of[4], (SECTIONS, TANGENTS, HD, D), HD ** -0.5, 0.25, ((0, 8), (3, 64)))
    layer_gain = jnp.clip(1.0 + 0.1 * jax.random.normal(key_of[5], (SECTIONS, D), jnp.float32), 0.5, 1.5)
    final_gain = jnp.clip(1.0 + 0.1 * jax.random.normal(key_of[6], (D,), jnp.float32), 0.5, 1.5)
    head = bell_draw(key_of[7], (D, CLASSES), D ** -0.5, 0.1875, ((1, 8),))
    return {"tokens": tokens, "w_qkv": w_qkv, "w_output": w_output, "tangent_value": tangent_value, "tangent_output": tangent_output, "layer_gain": layer_gain, "final_gain": final_gain, "head": head}


epsilon = 1e-06

def widen(array):
    return array.astype(jnp.float32)

def norm_jvp(primal, tangents, gains):
    average = lax.optimization_barrier(jnp.mean(primal, -1, keepdims=True))
    centred = primal - average
    inverse = lax.rsqrt(lax.optimization_barrier(jnp.mean(centred * centred, -1, keepdims=True)) + epsilon)
    dcentred = tangents - lax.optimization_barrier(jnp.mean(tangents, -1, keepdims=True))
    dinverse = -inverse ** 3 * lax.optimization_barrier(jnp.mean(centred * dcentred, -1, keepdims=True))
    return (centred * inverse * gains, (dcentred * inverse + centred * dinverse) * gains)

def layer_step(state, qkv_weight, out_weight, value_tangent, out_tangent, gains):
    resid = widen(state)
    normed_zero, normed_rest = norm_jvp(resid[0], resid[1:], gains)
    normed = jnp.concatenate([normed_zero[None], normed_rest]).astype(jnp.bfloat16)
    streams, batch, tokens_here, width = normed.shape
    projected = jnp.einsum('sbtd,de->sbte', widen(normed), widen(qkv_weight))
    extra_value = jnp.einsum('btd,kde->kbte', widen(normed[0]), widen(value_tangent))
    queries = projected[..., :HD]
    key_rows = projected[..., HD:2 * HD]
    values = projected[..., 2 * HD:]
    values = jnp.concatenate([values[:1], values[1:] + extra_value])
    shape_heads = (streams, batch, tokens_here, HEADS, HEAD)
    queries = queries.astype(jnp.bfloat16).reshape(shape_heads)
    key_rows = key_rows.astype(jnp.bfloat16).reshape(shape_heads)
    values = values.astype(jnp.bfloat16).reshape(shape_heads)
    factor = HEAD ** (-0.5)
    scores = jnp.einsum('bqhe,bkhe->bhqk', widen(queries[0]), widen(key_rows[0])) * factor
    probs = jax.nn.softmax(scores, -1)
    dscores = (jnp.einsum('sbqhe,bkhe->sbhqk', widen(queries[1:]), widen(key_rows[0])) + jnp.einsum('bqhe,sbkhe->sbhqk', widen(queries[0]), widen(key_rows[1:]))) * factor
    dprobs = probs * (dscores - lax.optimization_barrier(jnp.sum(probs * dscores, -1, keepdims=True)))
    probs_low = probs.astype(jnp.bfloat16)
    dprobs_low = dprobs.astype(jnp.bfloat16)
    attended_zero = jnp.einsum('bhqk,bkhe->bqhe', widen(probs_low), widen(values[0]))
    attended_rest = jnp.einsum('sbhqk,bkhe->sbqhe', widen(dprobs_low), widen(values[0])) + jnp.einsum('bhqk,sbkhe->sbqhe', widen(probs_low), widen(values[1:]))
    attended = jnp.concatenate([attended_zero[None], attended_rest]).astype(jnp.bfloat16)
    attended = attended.reshape(streams, batch, tokens_here, HD)
    output = jnp.einsum('sbte,ed->sbtd', widen(attended), widen(out_weight))
    extra_out = jnp.einsum('bte,ked->kbtd', widen(attended[0]), widen(out_tangent))
    output = jnp.concatenate([output[:1], output[1:] + extra_out])
    return (resid + output).astype(jnp.bfloat16)

def reference(tokens, w_qkv, w_output, tangent_value, tangent_output, layer_gain, final_gain, head):
    micro_count, image_count = (tokens.shape[0], tokens.shape[1])
    flat = tokens.reshape(micro_count * image_count, TOK, D)
    state = jnp.concatenate([flat[None], jnp.zeros((TANGENTS, micro_count * image_count, TOK, D), jnp.bfloat16)])
    for layer in range(N_SECTION):
        state = layer_step(state, w_qkv[layer], w_output[layer], tangent_value[layer], tangent_output[layer], layer_gain[layer])
    class_rows = widen(state[:, :, 0, :])
    final_zero, final_rest = norm_jvp(class_rows[0], class_rows[1:], final_gain)
    normed_final = jnp.concatenate([final_zero[None], final_rest]).astype(jnp.bfloat16)
    logits = jnp.einsum('sbd,dc->sbc', widen(normed_final), widen(head))
    mean_logits = logits[0].reshape(micro_count, image_count, CLASSES)
    variance = lax.optimization_barrier(jnp.sum(logits[1:] * logits[1:], 0)).reshape(micro_count, image_count, CLASSES)
    return (mean_logits, variance)
```

```python
import functools

import jax
import jax.numpy as jnp
from jax import lax
from jax.experimental import pallas as pl
from jax.experimental.pallas import tpu as pltpu
from jax.sharding import Mesh
from jax.sharding import PartitionSpec as P

HEADS = 8
HEAD = 64
TANGENTS = 2
HD = 512
PAIR = 2 * HEAD
PAIRS = HEADS // 2
SCALE = HEAD ** (-0.5)

epsilon = 1e-06

QKV = slice(0, 3 * HD)
TV = (slice(3 * HD, 4 * HD), slice(4 * HD, 5 * HD))
WO = slice(5 * HD, 6 * HD)
TO = (slice(6 * HD, 7 * HD), slice(7 * HD, 8 * HD))


VMEM_SPEC = pl.BlockSpec(memory_space=pltpu.VMEM)
SMEM_SPEC = pl.BlockSpec(memory_space=pltpu.SMEM)


def dot(left, right):
    return jnp.dot(left, right, preferred_element_type=jnp.float32)


def dot_t(left, right):
    return lax.dot_general(
        left, right, (((1,), (1,)), ((), ())), preferred_element_type=jnp.float32
    )


def row_mean(a):
    return jnp.sum(a, -1, keepdims=True) * (1.0 / a.shape[-1])


def head_masks(rows):
    lane = lax.broadcasted_iota(jnp.int32, (rows, PAIR), 1)
    return lane < HEAD, lane >= HEAD


def part(ref, which, pair):
    at = which * HD + pair * PAIR
    return ref[:, at : at + PAIR]


def masked(a, mask):
    return jnp.where(mask, a, jnp.zeros_like(a))


def working(step, plane):
    return (step - plane >= 0) & (step - plane < 2)


def primal_body(step, here, first_ref, *refs):
    x_ref, (g_ref, w_ref, out_ref, n_ref, qkv_ref, p_ref, att_ref) = refs[0], refs[-7:]
    plane = here[2]

    @pl.when(working(step, plane))
    def _():
        if step == 0:
            x = first_ref[0].astype(jnp.float32)
        else:
            x = x_ref[...].astype(jnp.float32)
        if step == 1:
            x = jnp.where(plane == 0, first_ref[1].astype(jnp.float32), x)
        c = x - row_mean(x)
        r = lax.rsqrt(row_mean(c * c) + epsilon)
        n = (c * r * g_ref[...]).astype(jnp.bfloat16)
        n_ref[...] = n
        qkv_ref[...] = dot(n, w_ref[:, QKV]).astype(jnp.bfloat16)
        masks = head_masks(x.shape[0])
        for pair in range(PAIRS):
            q, k, v = (part(qkv_ref, i, pair) for i in range(3))
            total = None
            for half in range(2):
                s = dot_t(masked(q, masks[half]), k) * SCALE
                e = jnp.exp(s - jnp.max(s, -1, keepdims=True))
                p = e / jnp.sum(e, -1, keepdims=True)
                p_ref[2 * pair + half] = p
                a = dot(p.astype(jnp.bfloat16), masked(v, masks[half]))
                total = a if total is None else total + a
            att_ref[:, pair * PAIR : (pair + 1) * PAIR] = total.astype(jnp.bfloat16)
        out_ref[...] = (x + dot_t(att_ref[...], w_ref[:, WO])).astype(jnp.bfloat16)


def tangent_body(which, step, here, first_ref, *refs):
    g_ref, w_ref, n_ref, qkv_ref, p_ref, att_ref, out_ref, mine, joined = refs[-9:]
    plane = here[2]

    @pl.when(working(step, plane))
    def _():
        if step == 0:
            x = first_ref[0].astype(jnp.float32)
            t = jnp.zeros_like(x)
        else:
            x = refs[0][...].astype(jnp.float32)
            t = refs[1][...].astype(jnp.float32)
        if step == 1:
            x = jnp.where(plane == 0, first_ref[1].astype(jnp.float32), x)
            t = jnp.where(plane == 0, jnp.zeros_like(t), t)
        c = x - row_mean(x)
        r = lax.rsqrt(row_mean(c * c) + epsilon)
        dc = t - row_mean(t)
        dr = -(r * r * r) * row_mean(c * dc)
        dn = ((dc * r + c * dr) * g_ref[...]).astype(jnp.bfloat16)
        mine[...] = dot(dn, w_ref[:, QKV]).astype(jnp.bfloat16)
        values = dot(dn, w_ref[:, 2 * HD : 3 * HD]) + dot(n_ref[...], w_ref[:, TV[which]])
        mine[:, 2 * HD :] = values.astype(jnp.bfloat16)
        masks = head_masks(x.shape[0])
        for pair in range(PAIRS):
            q0, k0, v0 = (part(qkv_ref, i, pair) for i in range(3))
            q1, k1, v1 = (part(mine, i, pair) for i in range(3))
            total = None
            for half in range(2):
                m = masks[half]
                ds = (dot_t(masked(q1, m), k0) + dot_t(masked(q0, m), k1)) * SCALE
                p = p_ref[2 * pair + half]
                dp = p * (ds - jnp.sum(p * ds, -1, keepdims=True))
                a = dot(dp.astype(jnp.bfloat16), masked(v0, m)) + dot(
                    p.astype(jnp.bfloat16), masked(v1, m)
                )
                total = a if total is None else total + a
            joined[:, pair * PAIR : (pair + 1) * PAIR] = total.astype(jnp.bfloat16)
        moved = dot_t(joined[...], w_ref[:, WO]) + dot_t(att_ref[...], w_ref[:, TO[which]])
        out_ref[...] = (t + moved).astype(jnp.bfloat16)


def cost(flops, bytes_accessed):
    return pl.CostEstimate(flops=flops, bytes_accessed=bytes_accessed, transcendentals=0)


def primal_layer(step, here, first, x, gain, weights):
    tokens, width = first.shape[1:]
    bf16 = jnp.bfloat16
    streams = (x,) if step else ()
    return pl.pallas_call(
        functools.partial(primal_body, step),
        out_shape=(
            jax.ShapeDtypeStruct((tokens, width), bf16),
            jax.ShapeDtypeStruct((tokens, width), bf16),
            jax.ShapeDtypeStruct((tokens, 3 * HD), bf16),
            jax.ShapeDtypeStruct((HEADS, tokens, tokens), jnp.float32),
            jax.ShapeDtypeStruct((tokens, HD), bf16),
        ),
        in_specs=[SMEM_SPEC] + [VMEM_SPEC] * (3 + len(streams)),
        out_specs=(VMEM_SPEC,) * 5,
        cost_estimate=cost(2 * tokens * width * 4 * HD, 1 << 20),
        compiler_params=pltpu.CompilerParams(vmem_limit_bytes=12 << 20),
        name="primal_layer",
    )(here, first, *streams, gain, weights)


def tangent_layer(which, step, here, first, x, t, gain, weights, saved):
    tokens, width = first.shape[1:]
    streams = (x, t) if step else ()
    return pl.pallas_call(
        functools.partial(tangent_body, which, step),
        out_shape=jax.ShapeDtypeStruct((tokens, width), jnp.bfloat16),
        in_specs=[SMEM_SPEC] + [VMEM_SPEC] * (7 + len(streams)),
        out_specs=VMEM_SPEC,
        scratch_shapes=[
            pltpu.VMEM((tokens, 3 * HD), jnp.bfloat16),
            pltpu.VMEM((tokens, HD), jnp.bfloat16),
        ],
        cost_estimate=cost(2 * tokens * width * 6 * HD, 1 << 20),
        compiler_params=pltpu.CompilerParams(vmem_limit_bytes=12 << 20),
        name=f"tangent_layer_{which}",
    )(here, first, *streams, gain, weights, *saved)


def assemble_body(here, *refs):
    pieces, out, sems = refs[:-2], refs[-2], refs[-1]
    core, y = here[0], here[1]
    back = 2 * core - 1
    rows = pieces[0].shape[0]
    half = rows // 2
    where = [y * rows]
    for step in range(1, 4):
        for offset in (back * step, -back * step):
            where.append(lax.rem(y + offset + 8, 8) * rows)
    far = lax.rem(y + 4, 8) * rows
    where += [far + half * core, far + half * (1 - core)]
    copies = []
    for i, piece in enumerate(pieces):
        at = pl.multiple_of(where[i], 64)
        copies.append(
            pltpu.make_async_copy(piece, out.at[pl.ds(at, piece.shape[0])], sems.at[i])
        )
    for copy in copies:
        copy.start()
    for copy in copies:
        copy.wait()


def assemble(here, pieces):
    rows = sum(p.shape[0] for p in pieces)
    columns = pieces[0].shape[1]
    return pl.pallas_call(
        assemble_body,
        out_shape=pltpu.VMEM((rows, columns), jnp.bfloat16),
        in_specs=[SMEM_SPEC] + [pl.BlockSpec(memory_space=pltpu.HBM)] * len(pieces),
        out_specs=VMEM_SPEC,
        scratch_shapes=[pltpu.SemaphoreType.DMA((len(pieces),))],
        cost_estimate=cost(1 << 20, 2 * rows * columns * 2),
        compiler_params=pltpu.CompilerParams(vmem_limit_bytes=12 << 20),
        name="assemble",
    )(here, *(pltpu.with_memory_space_constraint(p, pltpu.HBM) for p in pieces))


def core_swap(a):
    return lax.ppermute(a, "c", [(0, 1), (1, 0)])


def pairs_over(first, second, route):
    moves = []
    for i in range(first):
        for j in range(second):
            target = route(i, j)
            if target is not None:
                moves.append((i * second + j, target[0] * second + target[1]))
    return moves


def gathered(packed, here, core, beside):
    rows, columns = packed.shape
    share = lax.ppermute(packed, ("c", "zl"), pairs_over(2, 2, lambda c, z: (z, c)))
    line = lax.all_gather(share, "x", axis=0, tiled=True)
    other = core_swap(line)
    sizes = (4, 1, rows, columns)
    low = jnp.where(core == 0, line, other).reshape(sizes)
    high = jnp.where(core == 0, other, line).reshape(sizes)
    own = jnp.concatenate([low, high], 1).reshape(8 * rows, columns)
    ring = pairs_over(2, 8, lambda c, j: (c, (j + 1 - 2 * c) % 8))
    pieces, held, early = [own], own, beside
    for step in range(1, 4):
        arrived = lax.ppermute(held, ("c", "y"), ring)
        held, early = lax.optimization_barrier((arrived, early))
        if step == 1:
            beside = early
        else:
            pieces.append(early)
        early = core_swap(held)
        pieces.append(held)
    half = own.shape[0] // 2
    held = lax.ppermute(jnp.where(core == 0, held[:half], held[half:]), ("c", "y"), ring)
    held, early = lax.optimization_barrier((held, early))
    pieces += [early, held, core_swap(held)]
    return assemble(here, pieces), beside


def norm_jvp(primal, tangents, gains):
    average = jnp.mean(primal, -1, keepdims=True)
    centred = primal - average
    inverse = lax.rsqrt(jnp.mean(centred * centred, -1, keepdims=True) + epsilon)
    dcentred = tangents - jnp.mean(tangents, -1, keepdims=True)
    dinverse = -(inverse**3) * jnp.mean(centred * dcentred, -1, keepdims=True)
    return (centred * inverse * gains, (dcentred * inverse + centred * dinverse) * gains)


def shards(tokens, w_qkv, w_output, tangent_value, tangent_output, layer_gain, final_gain, head):
    core = lax.axis_index("c")
    plane_low = lax.axis_index("zl")
    plane = 2 * lax.axis_index("zh") + plane_low
    here = jnp.stack([core, lax.axis_index("y"), plane]).astype(jnp.int32)
    micro, _, length, width = tokens.shape
    packed = jnp.concatenate(
        [
            w_qkv[0],
            tangent_value[0, 0],
            tangent_value[0, 1],
            w_output[0].T,
            tangent_output[0, 0].T,
            tangent_output[0, 1].T,
        ],
        axis=1,
    )
    images = tokens.reshape(micro, length, width)
    beside = (core_swap(layer_gain), lax.ppermute(images, ("c", "zl"), [(3, 2)]))
    weights, (other_gain, other_images) = gathered(packed, here, core, beside)
    gain = jnp.where(core == plane_low, layer_gain, other_gain)
    images = jnp.where(core == 0, images, other_images)

    stages = 8
    streams = (None,) * (1 + TANGENTS)
    class_rows = []
    for step in range(stages + micro - 1):
        route = [(s, s + 1) for s in range(stages - 1) if 0 <= step - s < micro]
        out, *saved = primal_layer(step, here, images, streams[0], gain, weights)
        results, moved = [out], []
        if route:
            moved.append(lax.ppermute(out, ("zh", "zl"), route))
        for which in range(TANGENTS):
            out = tangent_layer(
                which, step, here, images, streams[0], streams[1 + which], gain, weights, saved
            )
            results.append(out)
            if route:
                moved.append(lax.ppermute(out, ("zh", "zl"), route))
        streams = tuple(moved)
        if step >= stages - 1:
            class_rows.append(jnp.stack([r[0] for r in results]))
    features = jnp.stack(class_rows, 1)
    everyone = lax.all_gather(features, ("zh", "c", "zl"))
    last = everyone.shape[0] - 1
    features = lax.dynamic_index_in_dim(everyone, last - 2 + 2 * plane_low, 0, keepdims=False)
    widened = features.astype(jnp.float32)
    final_zero, final_rest = norm_jvp(widened[0], widened[1:], final_gain)
    normed_final = jnp.concatenate([final_zero[None], final_rest]).astype(jnp.bfloat16)
    logits = jnp.einsum("sbd,dc->sbc", normed_final, head, preferred_element_type=jnp.float32)
    mean_logits = logits[0][:, None, :]
    variance = jnp.sum(logits[1:] * logits[1:], 0)[:, None, :]
    return (mean_logits, variance)


def solution(mesh):
    sizes = (4, 2, 8, 4, 2)
    split = Mesh(mesh.devices.reshape(sizes), ("zh", "c", "y", "x", "zl"))
    section, dp = ("zh", "c"), ("y", "x", "zl")
    return jax.shard_map(
        shards,
        mesh=split,
        in_specs=(
            P(None, dp, None, None),
            P(section, dp, None),
            P(section, None, dp),
            P(section, None, dp, None),
            P(section, None, None, dp),
            P(section, None),
            P(),
            P(None, section),
        ),
        out_specs=(P(None, dp, section), P(None, dp, section)),
        check_vma=False,
    )
```

```python
import functools

import jax
import jax.numpy as jnp
from jax import lax
from jax.experimental import pallas as pl
from jax.experimental.pallas import tpu as pltpu
from jax.sharding import Mesh
from jax.sharding import PartitionSpec as P

HEADS = 8
HEAD = 64
TANGENTS = 2
HD = 512
PAIR = 2 * HEAD
PAIRS = HEADS // 2
SCALE = HEAD ** (-0.5)

epsilon = 1e-06

QKV = slice(0, 3 * HD)
TV = (slice(3 * HD, 4 * HD), slice(4 * HD, 5 * HD))
WO = slice(5 * HD, 6 * HD)
TO = (slice(6 * HD, 7 * HD), slice(7 * HD, 8 * HD))


VMEM_SPEC = pl.BlockSpec(memory_space=pltpu.VMEM)
HBM_SPEC = pl.BlockSpec(memory_space=pltpu.HBM)
SMEM_SPEC = pl.BlockSpec(memory_space=pltpu.SMEM)


def dot(left, right):
    return jnp.dot(left, right, preferred_element_type=jnp.float32)


def dot_t(left, right):
    return lax.dot_general(
        left, right, (((1,), (1,)), ((), ())), preferred_element_type=jnp.float32
    )


def row_mean(a):
    return jnp.sum(a, -1, keepdims=True) * (1.0 / a.shape[-1])


def head_masks(rows):
    lane = lax.broadcasted_iota(jnp.int32, (rows, PAIR), 1)
    return lane < HEAD, lane >= HEAD


def part(ref, which, pair):
    at = which * HD + pair * PAIR
    return ref[:, at : at + PAIR]


def masked(a, mask):
    return jnp.where(mask, a, jnp.zeros_like(a))


def working(step, plane):
    return (step - plane >= 0) & (step - plane < 2)


def entering(step, here, images, stream, t_stream=None):
    core, plane = here[0], here[2]
    if step < 2:
        own, other = images
        x = jnp.where(core == 0, own[step], other[step]).astype(jnp.float32)
        t = jnp.zeros_like(x)
        if step == 1:
            x = jnp.where(plane == 0, x, stream[...].astype(jnp.float32))
            if t_stream is not None:
                t = jnp.where(plane == 0, t, t_stream[...].astype(jnp.float32))
        return x, t
    return (
        stream[...].astype(jnp.float32),
        None if t_stream is None else t_stream[...].astype(jnp.float32),
    )


def section_gain(here, own, other):
    return jnp.where(here[0] == lax.rem(here[2], 2), own[...], other[...])


def primal_body(step, here, *refs):
    own_gain, other_gain, w_ref, out_ref, n_ref, qkv_ref, p_ref, att_ref = refs[-8:]
    images, streams = refs[:2] if step < 2 else (), refs[2 if step < 2 else 0 : -8]

    @pl.when(working(step, here[2]))
    def _():
        x, _ = entering(step, here, images, *streams[:1] or (None,))
        gain = section_gain(here, own_gain, other_gain)
        c = x - row_mean(x)
        r = lax.rsqrt(row_mean(c * c) + epsilon)
        n = (c * r * gain).astype(jnp.bfloat16)
        n_ref[...] = n
        qkv_ref[...] = dot(n, w_ref[:, QKV]).astype(jnp.bfloat16)
        masks = head_masks(x.shape[0])
        for pair in range(PAIRS):
            q, k, v = (part(qkv_ref, i, pair) for i in range(3))
            total = None
            for half in range(2):
                s = dot_t(masked(q, masks[half]), k) * SCALE
                e = jnp.exp(s - jnp.max(s, -1, keepdims=True))
                p = e / jnp.sum(e, -1, keepdims=True)
                p_ref[2 * pair + half] = p
                a = dot(p.astype(jnp.bfloat16), masked(v, masks[half]))
                total = a if total is None else total + a
            att_ref[:, pair * PAIR : (pair + 1) * PAIR] = total.astype(jnp.bfloat16)
        out_ref[...] = (x + dot_t(att_ref[...], w_ref[:, WO])).astype(jnp.bfloat16)


def tangent_body(which, step, here, *refs):
    own_gain, other_gain, w_ref, n_ref, qkv_ref, p_ref, att_ref, out_ref, mine, joined = refs[-10:]
    images, streams = refs[:2] if step < 2 else (), refs[2 if step < 2 else 0 : -10]

    @pl.when(working(step, here[2]))
    def _():
        x, t = entering(step, here, images, *(streams or (None, None)))
        gain = section_gain(here, own_gain, other_gain)
        c = x - row_mean(x)
        r = lax.rsqrt(row_mean(c * c) + epsilon)
        dc = t - row_mean(t)
        dr = -(r * r * r) * row_mean(c * dc)
        dn = ((dc * r + c * dr) * gain).astype(jnp.bfloat16)
        mine[...] = dot(dn, w_ref[:, QKV]).astype(jnp.bfloat16)
        values = dot(dn, w_ref[:, 2 * HD : 3 * HD]) + dot(n_ref[...], w_ref[:, TV[which]])
        mine[:, 2 * HD :] = values.astype(jnp.bfloat16)
        masks = head_masks(x.shape[0])
        for pair in range(PAIRS):
            q0, k0, v0 = (part(qkv_ref, i, pair) for i in range(3))
            q1, k1, v1 = (part(mine, i, pair) for i in range(3))
            total = None
            for half in range(2):
                m = masks[half]
                ds = (dot_t(masked(q1, m), k0) + dot_t(masked(q0, m), k1)) * SCALE
                p = p_ref[2 * pair + half]
                dp = p * (ds - jnp.sum(p * ds, -1, keepdims=True))
                a = dot(dp.astype(jnp.bfloat16), masked(v0, m)) + dot(
                    p.astype(jnp.bfloat16), masked(v1, m)
                )
                total = a if total is None else total + a
            joined[:, pair * PAIR : (pair + 1) * PAIR] = total.astype(jnp.bfloat16)
        moved = dot_t(joined[...], w_ref[:, WO]) + dot_t(att_ref[...], w_ref[:, TO[which]])
        out_ref[...] = (t + moved).astype(jnp.bfloat16)


def cost(flops, bytes_accessed):
    return pl.CostEstimate(flops=flops, bytes_accessed=bytes_accessed, transcendentals=0)


def vmem(shape, dtype=jnp.bfloat16):
    return pltpu.VMEM(shape, dtype)


def in_hbm(a):
    return pltpu.with_memory_space_constraint(a, pltpu.HBM)


def limit(mib=4):
    return pltpu.CompilerParams(vmem_limit_bytes=mib << 20)


def primal_layer(step, here, images, x, gains, weights):
    tokens, width = images[0].shape[1:]
    bf16 = jnp.bfloat16
    streams = (*(images if step < 2 else ()), *((x,) if step else ()))
    return pl.pallas_call(
        functools.partial(primal_body, step),
        out_shape=(
            jax.ShapeDtypeStruct((tokens, width), bf16),
            jax.ShapeDtypeStruct((tokens, width), bf16),
            jax.ShapeDtypeStruct((tokens, 3 * HD), bf16),
            jax.ShapeDtypeStruct((HEADS, tokens, tokens), jnp.float32),
            jax.ShapeDtypeStruct((tokens, HD), bf16),
        ),
        in_specs=[SMEM_SPEC] + [VMEM_SPEC] * (3 + len(streams)),
        out_specs=(VMEM_SPEC,) * 5,
        cost_estimate=cost(2 * tokens * width * 4 * HD, 1 << 20),
        compiler_params=limit(12),
        name="primal_layer",
    )(here, *streams, *gains, weights)


def tangent_layer(which, step, here, images, x, t, gains, weights, saved):
    tokens, width = images[0].shape[1:]
    streams = (*(images if step < 2 else ()), *((x, t) if step else ()))
    return pl.pallas_call(
        functools.partial(tangent_body, which, step),
        out_shape=jax.ShapeDtypeStruct((tokens, width), jnp.bfloat16),
        in_specs=[SMEM_SPEC] + [VMEM_SPEC] * (7 + len(streams)),
        out_specs=VMEM_SPEC,
        scratch_shapes=[vmem((tokens, 3 * HD)), vmem((tokens, HD))],
        cost_estimate=cost(2 * tokens * width * 6 * HD, 1 << 20),
        compiler_params=limit(12),
        name=f"tangent_layer_{which}",
    )(here, *streams, *gains, weights, *saved)


def copied(pairs, sems):
    copies = [pltpu.make_async_copy(a, b, sems.at[i]) for i, (a, b) in enumerate(pairs)]
    for copy in copies:
        copy.start()
    for copy in copies:
        copy.wait()


def pack_body(qkv, value, output, tangent_output, out, sems):
    pairs = [(qkv.at[0], out.at[:, QKV]), (output.at[0], out.at[:, WO])]
    for which in range(TANGENTS):
        pairs.append((value.at[0, which], out.at[:, TV[which]]))
        pairs.append((tangent_output.at[0, which], out.at[:, TO[which]]))
    copied(pairs, sems)


def pack(w_qkv, tangent_value, w_output, tangent_output):
    shares = (w_qkv, tangent_value, w_output.swapaxes(1, 2), tangent_output.swapaxes(2, 3))
    return pl.pallas_call(
        pack_body,
        out_shape=vmem((w_qkv.shape[1], 8 * HD)),
        in_specs=[HBM_SPEC] * 4,
        out_specs=VMEM_SPEC,
        scratch_shapes=[pltpu.SemaphoreType.DMA((2 + 2 * TANGENTS,))],
        compiler_params=limit(),
        name="pack",
    )(*map(in_hbm, shares))


def line_body(*refs):
    parts, out, sems = refs[:-2], refs[-2], refs[-1]
    rows = parts[0].shape[0]
    copied([(p, out.at[pl.ds(i * rows, rows)]) for i, p in enumerate(parts)], sems)


def line_up(parts):
    rows, columns = parts[0].shape
    return pl.pallas_call(
        line_body,
        out_shape=vmem((len(parts) * rows, columns)),
        in_specs=[VMEM_SPEC] * len(parts),
        out_specs=VMEM_SPEC,
        scratch_shapes=[pltpu.SemaphoreType.DMA((len(parts),))],
        compiler_params=limit(),
        name="line_up",
    )(*parts)


def halves_body(up, down, first, second, sems):
    half = first.shape[0]
    copied([(up.at[pl.ds(0, half)], first), (down.at[pl.ds(half, half)], second)], sems)


def halves(up, down):
    rows, columns = up.shape
    return pl.pallas_call(
        halves_body,
        out_shape=(vmem((rows // 2, columns)),) * 2,
        in_specs=[VMEM_SPEC] * 2,
        out_specs=(VMEM_SPEC,) * 2,
        scratch_shapes=[pltpu.SemaphoreType.DMA((2,))],
        compiler_params=limit(),
        name="halves",
    )(up, down)


LINE = (0, -1, 1, 2)


def assemble_body(places, aliased, here, *refs):
    pieces = refs[int(aliased) : -2]
    out, sems = refs[-2:]
    core, y, x = here[0], here[1], here[3]
    pairs = []
    for piece, (rise, swapped, first) in zip(pieces, places, strict=True):
        rows = 16
        side = 1 - core if swapped else core
        for i in range(piece.shape[0] // rows):
            column = lax.rem(x + LINE[first + i] + 4, 4)
            at = (lax.rem(y + rise + 8, 8) * 4 + column) * 2 + side
            at = pl.multiple_of(at * rows, rows)
            pairs.append((piece.at[pl.ds(i * rows, rows)], out.at[pl.ds(at, rows)]))
    copied(pairs, sems)


def assemble(here, base, places, pieces):
    columns = pieces[0].shape[1]
    given, piece_spec = ([], HBM_SPEC) if base is None else ([base], VMEM_SPEC)
    if base is None:
        pieces = [in_hbm(p) for p in pieces]
    copies = sum(p.shape[0] for p in pieces) // 16
    return pl.pallas_call(
        functools.partial(assemble_body, places, base is not None),
        out_shape=vmem((1024, columns)),
        in_specs=[SMEM_SPEC] + [VMEM_SPEC] * len(given) + [piece_spec] * len(pieces),
        out_specs=VMEM_SPEC,
        input_output_aliases={1: 0} if given else {},
        scratch_shapes=[pltpu.SemaphoreType.DMA((copies,))],
        cost_estimate=cost(1 << 20, 32 * copies * columns * 2),
        compiler_params=limit(),
        name="assemble",
    )(here, *given, *pieces)


def core_swap(a):
    return lax.ppermute(a, "c", [(0, 1), (1, 0)])


def gathered(packed, here, beside):
    def moves(d):
        cells = [(c, x, z) for c in range(2) for x in range(4) for z in range(2)]
        return [(8 * c + 2 * x + z, 8 * z + 2 * ((x + d) % 4) + c) for c, x, z in cells]

    line = line_up([lax.ppermute(packed, ("c", "x", "zl"), moves(d)) for d in (0, 1, -1, 2)])
    up_route = [(j, (j + 1) % 8) for j in range(8)]
    down_route = [(j, (j - 1) % 8) for j in range(8)]
    up = down = line
    early = (core_swap(line), *beside)
    pieces, places = [line], [(0, False, 0)]
    base = None
    for step in range(1, 5):
        if step == 4:
            up, down = halves(up, down)
        arrived = (lax.ppermute(up, "y", up_route), lax.ppermute(down, "y", down_route))
        if step == 4:
            base = assemble(here, None, places, pieces)
            arrived, early, base = lax.optimization_barrier((arrived, early, base))
            pieces, places = [], []
        else:
            arrived, early = lax.optimization_barrier((arrived, early))
        if step == 1:
            beside, early = early[1:], early[:1]
            places.append((0, True, 0))
        else:
            places += [(1 - step, True, 0), (step - 1, True, 0)]
        pieces += early
        up, down = arrived
        pieces += [up, down]
        places += [(-step, False, 0), (step, False, 0 if step < 4 else 2)]
        early = (core_swap(up), core_swap(down))
    pieces += early
    places += [(-4, True, 0), (4, True, 2)]
    return assemble(here, base, tuple(places), pieces), beside


def rows_body(*refs):
    streams, out = refs[:-1], refs[-1]
    out[...] = jnp.zeros_like(out)
    for i, stream in enumerate(streams):
        out[i : i + 1] = stream[0:1]


def class_rows(streams):
    return pl.pallas_call(
        rows_body,
        out_shape=vmem((8, streams[0].shape[1])),
        in_specs=[VMEM_SPEC] * len(streams),
        out_specs=VMEM_SPEC,
        compiler_params=limit(),
        name="class_rows",
    )(*streams)


def sum_body(*refs):
    total = refs[0][...]
    for ref in refs[1:-1]:
        total = total + ref[...]
    refs[-1][...] = total


def one_of(parts):
    return pl.pallas_call(
        sum_body,
        out_shape=vmem(parts[0].shape),
        in_specs=[VMEM_SPEC] * len(parts),
        out_specs=VMEM_SPEC,
        compiler_params=limit(),
        name="one_of",
    )(*parts)


def norm_jvp(primal, tangents, gains):
    average = jnp.mean(primal, -1, keepdims=True)
    centred = primal - average
    inverse = lax.rsqrt(jnp.mean(centred * centred, -1, keepdims=True) + epsilon)
    dcentred = tangents - jnp.mean(tangents, -1, keepdims=True)
    dinverse = -(inverse**3) * jnp.mean(centred * dcentred, -1, keepdims=True)
    return (centred * inverse * gains, (dcentred * inverse + centred * dinverse) * gains)


def shards(tokens, w_qkv, w_output, tangent_value, tangent_output, layer_gain, final_gain, head):
    core = lax.axis_index("c")
    plane_low = lax.axis_index("zl")
    plane = 2 * lax.axis_index("zh") + plane_low
    here = jnp.stack([core, lax.axis_index("y"), plane, lax.axis_index("x")]).astype(jnp.int32)
    micro, _, length, width = tokens.shape
    images = tokens.reshape(micro, length, width)
    beside = (core_swap(layer_gain), lax.ppermute(images, ("c", "zl"), [(3, 2)]))
    packed = pack(w_qkv, tangent_value, w_output, tangent_output)
    weights, (other_gain, other_images) = gathered(packed, here, beside)
    gains, images = (layer_gain, other_gain), (images, other_images)

    stages = 8
    streams = (None,) * (1 + TANGENTS)
    last = []
    for step in range(stages + micro - 1):
        route = [(s, s + 1) for s in range(stages - 1) if 0 <= step - s < micro]
        out, *saved = primal_layer(step, here, images, streams[0], gains, weights)
        results, moved = [out], []
        if route:
            moved.append(lax.ppermute(out, ("zh", "zl"), route))
        for which in range(TANGENTS):
            out = tangent_layer(
                which, step, here, images, streams[0], streams[1 + which], gains, weights, saved
            )
            results.append(out)
            if route:
                moved.append(lax.ppermute(out, ("zh", "zl"), route))
        streams = tuple(moved)
        if step >= stages - 1:
            last += results
    rows = class_rows(last)
    sent = [
        lax.ppermute(rows, ("zh", "c", "zl"), [(13, 4 * i), (15, 4 * i + 3)]) for i in range(4)
    ]
    mine = one_of(sent)
    mine = jnp.where(core == plane_low, mine, core_swap(mine))
    features = mine[: micro * (1 + TANGENTS)].reshape(micro, 1 + TANGENTS, width).swapaxes(0, 1)
    widened = features.astype(jnp.float32)
    final_zero, final_rest = norm_jvp(widened[0], widened[1:], final_gain)
    normed_final = jnp.concatenate([final_zero[None], final_rest]).astype(jnp.bfloat16)
    logits = jnp.einsum("sbd,dc->sbc", normed_final, head, preferred_element_type=jnp.float32)
    mean_logits = logits[0][:, None, :]
    variance = jnp.sum(logits[1:] * logits[1:], 0)[:, None, :]
    return (mean_logits, variance)


def solution(mesh):
    sizes = (4, 2, 8, 4, 2)
    split = Mesh(mesh.devices.reshape(sizes), ("zh", "c", "y", "x", "zl"))
    section, dp = ("zh", "c"), ("y", "x", "zl")
    return jax.shard_map(
        shards,
        mesh=split,
        in_specs=(
            P(None, dp, None, None),
            P(section, dp, None),
            P(section, None, dp),
            P(section, None, dp, None),
            P(section, None, None, dp),
            P(section, None),
            P(),
            P(None, section),
        ),
        out_specs=(P(None, dp, section), P(None, dp, section)),
        check_vma=False,
    )
```

```python
import functools

import jax
import jax.numpy as jnp
from jax import lax
from jax.experimental import pallas as pl
from jax.experimental.pallas import tpu as pltpu
from jax.sharding import Mesh
from jax.sharding import PartitionSpec as P

HEADS = 8
HEAD = 64
TANGENTS = 2
HD = 512
PAIR = 2 * HEAD
PAIRS = HEADS // 2
SCALE = HEAD ** (-0.5)

epsilon = 1e-06

QKV = slice(0, 3 * HD)
TV = (slice(3 * HD, 4 * HD), slice(4 * HD, 5 * HD))
WO = slice(5 * HD, 6 * HD)
TO = (slice(6 * HD, 7 * HD), slice(7 * HD, 8 * HD))


VMEM_SPEC = pl.BlockSpec(memory_space=pltpu.VMEM)
HBM_SPEC = pl.BlockSpec(memory_space=pltpu.HBM)
SMEM_SPEC = pl.BlockSpec(memory_space=pltpu.SMEM)


def dot(left, right):
    return jnp.dot(left, right, preferred_element_type=jnp.float32)


def dot_t(left, right):
    return lax.dot_general(
        left, right, (((1,), (1,)), ((), ())), preferred_element_type=jnp.float32
    )


def row_mean(a):
    return jnp.sum(a, -1, keepdims=True) * (1.0 / a.shape[-1])


def head_masks(rows):
    lane = lax.broadcasted_iota(jnp.int32, (rows, PAIR), 1)
    return lane < HEAD, lane >= HEAD


def part(ref, which, pair):
    at = which * HD + pair * PAIR
    return ref[:, at : at + PAIR]


def masked(a, mask):
    return jnp.where(mask, a, jnp.zeros_like(a))


def working(step, plane):
    return (step - plane >= 0) & (step - plane < 2)


def entering(step, here, images, stream, t_stream=None):
    core, plane = here[0], here[2]
    if step < 2:
        own, other = images
        x = jnp.where(core == 0, own[step], other[step]).astype(jnp.float32)
        t = jnp.zeros_like(x)
        if step == 1:
            x = jnp.where(plane == 0, x, stream[...].astype(jnp.float32))
            if t_stream is not None:
                t = jnp.where(plane == 0, t, t_stream[...].astype(jnp.float32))
        return x, t
    return (
        stream[...].astype(jnp.float32),
        None if t_stream is None else t_stream[...].astype(jnp.float32),
    )


def section_gain(here, own, other):
    return jnp.where(here[0] == lax.rem(here[2], 2), own[...], other[...])


def primal_body(step, here, *refs):
    own_gain, other_gain, w_ref, out_ref, n_ref, qkv_ref, p_ref, att_ref = refs[-8:]
    images, streams = refs[:2] if step < 2 else (), refs[2 if step < 2 else 0 : -8]

    @pl.when(working(step, here[2]))
    def _():
        x, _ = entering(step, here, images, *streams[:1] or (None,))
        gain = section_gain(here, own_gain, other_gain)
        c = x - row_mean(x)
        r = lax.rsqrt(row_mean(c * c) + epsilon)
        n = (c * r * gain).astype(jnp.bfloat16)
        n_ref[...] = n
        qkv_ref[...] = dot(n, w_ref[:, QKV]).astype(jnp.bfloat16)
        masks = head_masks(x.shape[0])
        for pair in range(PAIRS):
            q, k, v = (part(qkv_ref, i, pair) for i in range(3))
            total = None
            for half in range(2):
                s = dot_t(masked(q, masks[half]), k) * SCALE
                e = jnp.exp(s - jnp.max(s, -1, keepdims=True))
                p = e / jnp.sum(e, -1, keepdims=True)
                p_ref[2 * pair + half] = p
                a = dot(p.astype(jnp.bfloat16), masked(v, masks[half]))
                total = a if total is None else total + a
            att_ref[:, pair * PAIR : (pair + 1) * PAIR] = total.astype(jnp.bfloat16)
        out_ref[...] = (x + dot_t(att_ref[...], w_ref[:, WO])).astype(jnp.bfloat16)


def shared_body(step, here, w_ref, n_ref, att_ref, values_ref, outs_ref):
    @pl.when(working(step, here[2]))
    def _():
        for which in range(TANGENTS):
            values_ref[which] = dot(n_ref[...], w_ref[:, TV[which]])
            outs_ref[which] = dot_t(att_ref[...], w_ref[:, TO[which]])


def tangent_body(which, step, here, *refs):
    own_gain, other_gain, w_ref, qkv_ref, p_ref, values_ref, outs_ref, out_ref, mine, joined = refs[-10:]
    images, streams = refs[:2] if step < 2 else (), refs[2 if step < 2 else 0 : -10]

    @pl.when(working(step, here[2]))
    def _():
        x, t = entering(step, here, images, *(streams or (None, None)))
        gain = section_gain(here, own_gain, other_gain)
        c = x - row_mean(x)
        r = lax.rsqrt(row_mean(c * c) + epsilon)
        dc = t - row_mean(t)
        dr = -(r * r * r) * row_mean(c * dc)
        dn = ((dc * r + c * dr) * gain).astype(jnp.bfloat16)
        mine[:, : 2 * HD] = dot(dn, w_ref[:, : 2 * HD]).astype(jnp.bfloat16)
        values = dot(dn, w_ref[:, 2 * HD : 3 * HD]) + values_ref[which]
        mine[:, 2 * HD :] = values.astype(jnp.bfloat16)
        masks = head_masks(x.shape[0])
        for pair in range(PAIRS):
            q0, k0, v0 = (part(qkv_ref, i, pair) for i in range(3))
            q1, k1, v1 = (part(mine, i, pair) for i in range(3))
            total = None
            for half in range(2):
                m = masks[half]
                ds = (dot_t(masked(q1, m), k0) + dot_t(masked(q0, m), k1)) * SCALE
                p = p_ref[2 * pair + half]
                dp = p * (ds - jnp.sum(p * ds, -1, keepdims=True))
                a = dot(dp.astype(jnp.bfloat16), masked(v0, m)) + dot(
                    p.astype(jnp.bfloat16), masked(v1, m)
                )
                total = a if total is None else total + a
            joined[:, pair * PAIR : (pair + 1) * PAIR] = total.astype(jnp.bfloat16)
        moved = dot_t(joined[...], w_ref[:, WO]) + outs_ref[which]
        out_ref[...] = (t + moved).astype(jnp.bfloat16)


def cost(flops, bytes_accessed):
    return pl.CostEstimate(flops=flops, bytes_accessed=bytes_accessed, transcendentals=0)


def vmem(shape, dtype=jnp.bfloat16):
    return pltpu.VMEM(shape, dtype)


def in_hbm(a):
    return pltpu.with_memory_space_constraint(a, pltpu.HBM)


def limit(mib=4):
    return pltpu.CompilerParams(vmem_limit_bytes=mib << 20)


def primal_layer(step, here, images, x, gains, weights):
    tokens, width = images[0].shape[1:]
    bf16 = jnp.bfloat16
    streams = (*(images if step < 2 else ()), *((x,) if step else ()))
    return pl.pallas_call(
        functools.partial(primal_body, step),
        out_shape=(
            jax.ShapeDtypeStruct((tokens, width), bf16),
            jax.ShapeDtypeStruct((tokens, width), bf16),
            jax.ShapeDtypeStruct((tokens, 3 * HD), bf16),
            jax.ShapeDtypeStruct((HEADS, tokens, tokens), jnp.float32),
            jax.ShapeDtypeStruct((tokens, HD), bf16),
        ),
        in_specs=[SMEM_SPEC] + [VMEM_SPEC] * (3 + len(streams)),
        out_specs=(VMEM_SPEC,) * 5,
        cost_estimate=cost(2 * tokens * width * 4 * HD, 1 << 20),
        compiler_params=limit(12),
        name="primal_layer",
    )(here, *streams, *gains, weights)


def shared_layer(step, here, weights, normed, attended):
    tokens, width = normed.shape
    return pl.pallas_call(
        functools.partial(shared_body, step),
        out_shape=(
            jax.ShapeDtypeStruct((TANGENTS, tokens, HD), jnp.float32),
            jax.ShapeDtypeStruct((TANGENTS, tokens, width), jnp.float32),
        ),
        in_specs=[SMEM_SPEC] + [VMEM_SPEC] * 3,
        out_specs=(VMEM_SPEC,) * 2,
        cost_estimate=cost(2 * tokens * width * 4 * HD, 1 << 20),
        compiler_params=limit(12),
        name="shared_layer",
    )(here, weights, normed, attended)


def tangent_layer(which, step, here, images, x, t, gains, weights, saved):
    tokens, width = images[0].shape[1:]
    streams = (*(images if step < 2 else ()), *((x, t) if step else ()))
    return pl.pallas_call(
        functools.partial(tangent_body, which, step),
        out_shape=jax.ShapeDtypeStruct((tokens, width), jnp.bfloat16),
        in_specs=[SMEM_SPEC] + [VMEM_SPEC] * (7 + len(streams)),
        out_specs=VMEM_SPEC,
        scratch_shapes=[vmem((tokens, 3 * HD)), vmem((tokens, HD))],
        cost_estimate=cost(2 * tokens * width * 4 * HD, 1 << 20),
        compiler_params=limit(12),
    )(here, *streams, *gains, weights, *saved)


def copied(pairs, sems):
    copies = [pltpu.make_async_copy(a, b, sems.at[i]) for i, (a, b) in enumerate(pairs)]
    for copy in copies:
        copy.start()
    for copy in copies:
        copy.wait()


def pack_body(qkv, value, output, tangent_output, out, sems):
    pairs = [(qkv.at[0], out.at[:, QKV]), (output.at[0], out.at[:, WO])]
    for which in range(TANGENTS):
        pairs.append((value.at[0, which], out.at[:, TV[which]]))
        pairs.append((tangent_output.at[0, which], out.at[:, TO[which]]))
    copied(pairs, sems)


def pack(w_qkv, tangent_value, w_output, tangent_output):
    shares = (w_qkv, tangent_value, w_output.swapaxes(1, 2), tangent_output.swapaxes(2, 3))
    return pl.pallas_call(
        pack_body,
        out_shape=vmem((w_qkv.shape[1], 8 * HD)),
        in_specs=[HBM_SPEC] * 4,
        out_specs=VMEM_SPEC,
        scratch_shapes=[pltpu.SemaphoreType.DMA((2 + 2 * TANGENTS,))],
        compiler_params=limit(),
        name="pack",
    )(*map(in_hbm, shares))


def line_body(*refs):
    parts, out = refs[:-1], refs[-1]
    rows = parts[0].shape[0]
    for i, part in enumerate(parts):
        out[i * rows : (i + 1) * rows] = part[...]


def line_up(parts):
    rows, columns = parts[0].shape
    return pl.pallas_call(
        line_body,
        out_shape=vmem((len(parts) * rows, columns)),
        in_specs=[VMEM_SPEC] * len(parts),
        out_specs=VMEM_SPEC,
        compiler_params=limit(),
        name="line_up",
    )(*parts)


def halves_body(up, down, first, second):
    half = first.shape[0]
    first[...] = up[:half]
    second[...] = down[half:]


def halves(up, down):
    rows, columns = up.shape
    return pl.pallas_call(
        halves_body,
        out_shape=(vmem((rows // 2, columns)),) * 2,
        in_specs=[VMEM_SPEC] * 2,
        out_specs=(VMEM_SPEC,) * 2,
        compiler_params=limit(),
        name="halves",
    )(up, down)


LINE = (0, -1, 1, 2)


def assemble_body(places, aliased, here, *refs):
    count = len(places)
    pieces, out, sems = refs[int(aliased) :][:count], refs[int(aliased) + count], refs[int(aliased) + count + 1 :]
    core, y, x = here[0], here[1], here[3]
    pairs = []
    for piece, (rise, swapped, first) in zip(pieces, places, strict=True):
        rows = 16
        side = 1 - core if swapped else core
        for i in range(piece.shape[0] // rows):
            column = lax.rem(x + LINE[first + i] + 4, 4)
            at = (lax.rem(y + rise + 8, 8) * 4 + column) * 2 + side
            at = pl.multiple_of(at * rows, rows)
            if aliased:
                out[pl.ds(at, rows)] = piece[i * rows : (i + 1) * rows]
            else:
                pairs.append((piece.at[pl.ds(i * rows, rows)], out.at[pl.ds(at, rows)]))
    if not aliased:
        copied(pairs, sems[0])


def assemble(here, base, places, pieces):
    columns = pieces[0].shape[1]
    given, piece_spec = ([], HBM_SPEC) if base is None else ([base], VMEM_SPEC)
    if base is None:
        pieces = [in_hbm(p) for p in pieces]
    copies = sum(p.shape[0] for p in pieces) // 16
    return pl.pallas_call(
        functools.partial(assemble_body, places, base is not None),
        out_shape=vmem((1024, columns)),
        in_specs=[SMEM_SPEC] + [VMEM_SPEC] * len(given) + [piece_spec] * len(pieces),
        out_specs=VMEM_SPEC,
        input_output_aliases={1: 0} if given else {},
        scratch_shapes=[] if given else [pltpu.SemaphoreType.DMA((copies,))],
        cost_estimate=cost(1 << 20, 32 * copies * columns * 2),
        compiler_params=limit(),
        name="assemble",
    )(here, *given, *pieces)


def core_swap(a):
    return lax.ppermute(a, "c", [(0, 1), (1, 0)])


def gathered(packed, here, gain, images):
    def moves(d):
        cells = [(c, x, z) for c in range(2) for x in range(4) for z in range(2)]
        return [(8 * c + 2 * x + z, 8 * z + 2 * ((x + d) % 4) + c) for c, x, z in cells]

    def up_ring(a):
        return lax.ppermute(a, "y", [(j, (j + 1) % 8) for j in range(8)])

    def down_ring(a):
        return lax.ppermute(a, "y", [(j, (j - 1) % 8) for j in range(8)])

    def to_pair(a):
        return lax.ppermute(a, ("c", "zl"), [(3, 2)])

    line = line_up([lax.ppermute(packed, ("c", "x", "zl"), moves(d)) for d in (0, 1, -1, 2)])
    up = down = line
    early = (core_swap(line), core_swap(gain), to_pair(images))
    pieces, places = [line], [(0, False, 0)]
    base = None
    for step in range(1, 5):
        if step == 4:
            up, down = halves(up, down)
        arrived = (up_ring(up), down_ring(down))
        if step == 4:
            base = assemble(here, None, places, pieces)
            arrived, early, base = lax.optimization_barrier((arrived, early, base))
            pieces, places = [], []
        else:
            arrived, early = lax.optimization_barrier((arrived, early))
        if step == 1:
            beside, early = early[1:], early[:1]
            places.append((0, True, 0))
        else:
            places += [(1 - step, True, 0), (step - 1, True, 0)]
        pieces += early
        up, down = arrived
        pieces += [up, down]
        places += [(-step, False, 0), (step, False, 0 if step < 4 else 2)]
        early = (core_swap(up), core_swap(down))
    pieces += early
    places += [(-4, True, 0), (4, True, 2)]
    return assemble(here, base, tuple(places), pieces), beside


def rows_body(*refs):
    streams, out = refs[:-1], refs[-1]
    out[...] = jnp.zeros_like(out)
    for i, stream in enumerate(streams):
        out[i : i + 1] = stream[0:1]


def class_rows(streams):
    return pl.pallas_call(
        rows_body,
        out_shape=vmem((8, streams[0].shape[1])),
        in_specs=[VMEM_SPEC] * len(streams),
        out_specs=VMEM_SPEC,
        compiler_params=limit(),
        name="class_rows",
    )(*streams)


def sum_body(*refs):
    total = refs[0][...]
    for ref in refs[1:-1]:
        total = total + ref[...]
    refs[-1][...] = total


def one_of(parts):
    return pl.pallas_call(
        sum_body,
        out_shape=vmem(parts[0].shape),
        in_specs=[VMEM_SPEC] * len(parts),
        out_specs=VMEM_SPEC,
        compiler_params=limit(),
        name="one_of",
    )(*parts)


def norm_jvp(primal, tangents, gains):
    average = jnp.mean(primal, -1, keepdims=True)
    centred = primal - average
    inverse = lax.rsqrt(jnp.mean(centred * centred, -1, keepdims=True) + epsilon)
    dcentred = tangents - jnp.mean(tangents, -1, keepdims=True)
    dinverse = -(inverse**3) * jnp.mean(centred * dcentred, -1, keepdims=True)
    return (centred * inverse * gains, (dcentred * inverse + centred * dinverse) * gains)


def shards(tokens, w_qkv, w_output, tangent_value, tangent_output, layer_gain, final_gain, head):
    core = lax.axis_index("c")
    plane_low = lax.axis_index("zl")
    plane = 2 * lax.axis_index("zh") + plane_low
    here = jnp.stack([core, lax.axis_index("y"), plane, lax.axis_index("x")]).astype(jnp.int32)
    micro, _, length, width = tokens.shape
    images = tokens.reshape(micro, length, width)
    packed = pack(w_qkv, tangent_value, w_output, tangent_output)
    weights, (other_gain, other_images) = gathered(packed, here, layer_gain, images)
    gains, images = (layer_gain, other_gain), (images, other_images)

    stages = 8
    streams = (None,) * (1 + TANGENTS)
    last = []
    for step in range(stages + micro - 1):
        route = [(s, s + 1) for s in range(stages - 1) if 0 <= step - s < micro]
        out, normed, qkv, probs, attended = primal_layer(
            step, here, images, streams[0], gains, weights
        )
        saved = (qkv, probs, *shared_layer(step, here, weights, normed, attended))
        results, moved = [out], []
        if route:
            moved.append(lax.ppermute(out, ("zh", "zl"), route))
        for which in range(TANGENTS):
            out = tangent_layer(
                which, step, here, images, streams[0], streams[1 + which], gains, weights, saved
            )
            results.append(out)
            if route:
                moved.append(lax.ppermute(out, ("zh", "zl"), route))
        streams = tuple(moved)
        if step >= stages - 1:
            last += results
    rows = class_rows(last)
    sent = [
        lax.ppermute(rows, ("zh", "c", "zl"), [(13, 4 * i), (15, 4 * i + 3)]) for i in range(4)
    ]
    mine = one_of(sent)
    mine = jnp.where(core == plane_low, mine, core_swap(mine))
    features = mine[: micro * (1 + TANGENTS)].reshape(micro, 1 + TANGENTS, width).swapaxes(0, 1)
    widened = features.astype(jnp.float32)
    final_zero, final_rest = norm_jvp(widened[0], widened[1:], final_gain)
    normed_final = jnp.concatenate([final_zero[None], final_rest]).astype(jnp.bfloat16)
    logits = jnp.einsum("sbd,dc->sbc", normed_final, head, preferred_element_type=jnp.float32)
    mean_logits = logits[0][:, None, :]
    variance = jnp.sum(logits[1:] * logits[1:], 0)[:, None, :]
    return (mean_logits, variance)


def solution(mesh):
    sizes = (4, 2, 8, 4, 2)
    split = Mesh(mesh.devices.reshape(sizes), ("zh", "c", "y", "x", "zl"))
    section, dp = ("zh", "c"), ("y", "x", "zl")
    return jax.shard_map(
        shards,
        mesh=split,
        in_specs=(
            P(None, dp, None, None),
            P(section, dp, None),
            P(section, None, dp),
            P(section, None, dp, None),
            P(section, None, None, dp),
            P(section, None),
            P(),
            P(None, section),
        ),
        out_specs=(P(None, dp, section), P(None, dp, section)),
        check_vma=False,
    )
```

```python
import functools

import jax
import jax.numpy as jnp
from jax import lax
from jax.experimental import pallas as pl
from jax.experimental.pallas import tpu as pltpu
from jax.sharding import Mesh
from jax.sharding import PartitionSpec as P

HEADS = 8
HEAD = 64
TANGENTS = 2
HD = 512
PAIR = 2 * HEAD
PAIRS = HEADS // 2
SCALE = HEAD ** (-0.5)

epsilon = 1e-06

QKV = slice(0, 3 * HD)
TV = (slice(3 * HD, 4 * HD), slice(4 * HD, 5 * HD))
WO = slice(5 * HD, 6 * HD)
TO = (slice(6 * HD, 7 * HD), slice(7 * HD, 8 * HD))


VMEM_SPEC = pl.BlockSpec(memory_space=pltpu.VMEM)
HBM_SPEC = pl.BlockSpec(memory_space=pltpu.HBM)


def dot(left, right):
    return jnp.dot(left, right, preferred_element_type=jnp.float32)


def dot_t(left, right):
    return lax.dot_general(
        left, right, (((1,), (1,)), ((), ())), preferred_element_type=jnp.float32
    )


def row_mean(a):
    return jnp.sum(a, -1, keepdims=True) * (1.0 / a.shape[-1])


def head_masks(rows):
    lane = lax.broadcasted_iota(jnp.int32, (rows, PAIR), 1)
    return lane < HEAD, lane >= HEAD


def part(ref, which, pair):
    at = which * HD + pair * PAIR
    return ref[:, at : at + PAIR]


def masked(a, mask):
    return jnp.where(mask, a, jnp.zeros_like(a))


def plane_of_this():
    return 2 * lax.axis_index("zh") + lax.axis_index("zl")


def working(step, plane):
    return (step - plane >= 0) & (step - plane < 2)


def entering(step, plane, images, stream, t_stream=None):
    if step < 2:
        x = images[step].astype(jnp.float32)
        t = jnp.zeros_like(x)
        if step == 1:
            x = jnp.where(plane == 0, x, stream[...].astype(jnp.float32))
            if t_stream is not None:
                t = jnp.where(plane == 0, t, t_stream[...].astype(jnp.float32))
        return x, t
    return (
        stream[...].astype(jnp.float32),
        None if t_stream is None else t_stream[...].astype(jnp.float32),
    )


def primal_body(step, *refs):
    gain_ref, w_ref, out_ref, n_ref, qkv_ref, p_ref, att_ref = refs[-7:]
    images, streams = refs[0] if step < 2 else None, refs[1 if step < 2 else 0 : -7]
    plane = plane_of_this()

    @pl.when(working(step, plane))
    def _():
        x, _ = entering(step, plane, images, *streams[:1] or (None,))
        gain = gain_ref[...]
        c = x - row_mean(x)
        r = lax.rsqrt(row_mean(c * c) + epsilon)
        n = (c * r * gain).astype(jnp.bfloat16)
        n_ref[...] = n
        qkv_ref[...] = dot(n, w_ref[:, QKV]).astype(jnp.bfloat16)
        masks = head_masks(x.shape[0])
        for pair in range(PAIRS):
            q, k, v = (part(qkv_ref, i, pair) for i in range(3))
            total = None
            for half in range(2):
                s = dot_t(masked(q, masks[half]), k) * SCALE
                e = jnp.exp(s - jnp.max(s, -1, keepdims=True))
                p = e / jnp.sum(e, -1, keepdims=True)
                p_ref[2 * pair + half] = p
                a = dot(p.astype(jnp.bfloat16), masked(v, masks[half]))
                total = a if total is None else total + a
            att_ref[:, pair * PAIR : (pair + 1) * PAIR] = total.astype(jnp.bfloat16)
        out_ref[...] = (x + dot_t(att_ref[...], w_ref[:, WO])).astype(jnp.bfloat16)


def shared_body(step, w_ref, n_ref, att_ref, values_ref, outs_ref):
    @pl.when(working(step, plane_of_this()))
    def _():
        for which in range(TANGENTS):
            values_ref[which] = dot(n_ref[...], w_ref[:, TV[which]])
            outs_ref[which] = dot_t(att_ref[...], w_ref[:, TO[which]])


def tangent_body(which, step, *refs):
    gain_ref, w_ref, qkv_ref, p_ref, values_ref, outs_ref, out_ref, mine, joined = refs[-9:]
    images, streams = refs[0] if step < 2 else None, refs[1 if step < 2 else 0 : -9]
    plane = plane_of_this()

    @pl.when(working(step, plane))
    def _():
        x, t = entering(step, plane, images, *(streams or (None, None)))
        gain = gain_ref[...]
        c = x - row_mean(x)
        r = lax.rsqrt(row_mean(c * c) + epsilon)
        dc = t - row_mean(t)
        dr = -(r * r * r) * row_mean(c * dc)
        dn = ((dc * r + c * dr) * gain).astype(jnp.bfloat16)
        mine[:, : 2 * HD] = dot(dn, w_ref[:, : 2 * HD]).astype(jnp.bfloat16)
        values = dot(dn, w_ref[:, 2 * HD : 3 * HD]) + values_ref[which]
        mine[:, 2 * HD :] = values.astype(jnp.bfloat16)
        masks = head_masks(x.shape[0])
        for pair in range(PAIRS):
            q0, k0, v0 = (part(qkv_ref, i, pair) for i in range(3))
            q1, k1, v1 = (part(mine, i, pair) for i in range(3))
            total = None
            for half in range(2):
                m = masks[half]
                ds = (dot_t(masked(q1, m), k0) + dot_t(masked(q0, m), k1)) * SCALE
                p = p_ref[2 * pair + half]
                dp = p * (ds - jnp.sum(p * ds, -1, keepdims=True))
                a = dot(dp.astype(jnp.bfloat16), masked(v0, m)) + dot(
                    p.astype(jnp.bfloat16), masked(v1, m)
                )
                total = a if total is None else total + a
            joined[:, pair * PAIR : (pair + 1) * PAIR] = total.astype(jnp.bfloat16)
        moved = dot_t(joined[...], w_ref[:, WO]) + outs_ref[which]
        out_ref[...] = (t + moved).astype(jnp.bfloat16)


def cost(flops, bytes_accessed):
    return pl.CostEstimate(flops=flops, bytes_accessed=bytes_accessed, transcendentals=0)


def vmem(shape, dtype=jnp.bfloat16):
    return pltpu.VMEM(shape, dtype)


def in_hbm(a):
    return pltpu.with_memory_space_constraint(a, pltpu.HBM)


def limit(mib=4):
    return pltpu.CompilerParams(vmem_limit_bytes=mib << 20)


def primal_layer(step, images, x, gain, weights):
    tokens, width = images.shape[1:]
    bf16 = jnp.bfloat16
    given = (*((images,) if step < 2 else ()), *((x,) if step else ()), gain, weights)
    return pl.pallas_call(
        functools.partial(primal_body, step),
        out_shape=(
            jax.ShapeDtypeStruct((tokens, width), bf16),
            jax.ShapeDtypeStruct((tokens, width), bf16),
            jax.ShapeDtypeStruct((tokens, 3 * HD), bf16),
            jax.ShapeDtypeStruct((HEADS, tokens, tokens), jnp.float32),
            jax.ShapeDtypeStruct((tokens, HD), bf16),
        ),
        in_specs=[VMEM_SPEC] * len(given),
        out_specs=(VMEM_SPEC,) * 5,
        cost_estimate=cost(2 * tokens * width * 4 * HD, 1 << 20),
        compiler_params=limit(12),
        name="primal_layer",
    )(*given)


def shared_layer(step, weights, normed, attended):
    tokens, width = normed.shape
    return pl.pallas_call(
        functools.partial(shared_body, step),
        out_shape=(
            jax.ShapeDtypeStruct((TANGENTS, tokens, HD), jnp.float32),
            jax.ShapeDtypeStruct((TANGENTS, tokens, width), jnp.float32),
        ),
        in_specs=[VMEM_SPEC] * 3,
        out_specs=(VMEM_SPEC,) * 2,
        cost_estimate=cost(2 * tokens * width * 4 * HD, 1 << 20),
        compiler_params=limit(12),
        name="shared_layer",
    )(weights, normed, attended)


def tangent_layer(which, step, images, x, t, gain, weights, saved):
    tokens, width = images.shape[1:]
    given = (*((images,) if step < 2 else ()), *((x, t) if step else ()), gain, weights, *saved)
    return pl.pallas_call(
        functools.partial(tangent_body, which, step),
        out_shape=jax.ShapeDtypeStruct((tokens, width), jnp.bfloat16),
        in_specs=[VMEM_SPEC] * len(given),
        out_specs=VMEM_SPEC,
        scratch_shapes=[vmem((tokens, 3 * HD)), vmem((tokens, HD))],
        cost_estimate=cost(2 * tokens * width * 4 * HD, 1 << 20),
        compiler_params=limit(12),
    )(*given)


def copied(pairs, sems):
    copies = [pltpu.make_async_copy(a, b, sems.at[i]) for i, (a, b) in enumerate(pairs)]
    for copy in copies:
        copy.start()
    for copy in copies:
        copy.wait()


def pack_body(qkv, value, output, tangent_output, out, sems):
    pairs = [(qkv.at[0], out.at[:, QKV]), (output.at[0], out.at[:, WO])]
    for which in range(TANGENTS):
        pairs.append((value.at[0, which], out.at[:, TV[which]]))
        pairs.append((tangent_output.at[0, which], out.at[:, TO[which]]))
    copied(pairs, sems)


def pack(w_qkv, tangent_value, w_output, tangent_output):
    shares = (w_qkv, tangent_value, w_output.swapaxes(1, 2), tangent_output.swapaxes(2, 3))
    return pl.pallas_call(
        pack_body,
        out_shape=vmem((w_qkv.shape[1], 8 * HD)),
        in_specs=[HBM_SPEC] * 4,
        out_specs=VMEM_SPEC,
        scratch_shapes=[pltpu.SemaphoreType.DMA((2 + 2 * TANGENTS,))],
        compiler_params=limit(),
        name="pack",
    )(*map(in_hbm, shares))


def line_body(*refs):
    parts, out = refs[:-1], refs[-1]
    at = 0
    for part in parts:
        out[at : at + part.shape[0]] = part[...]
        at += part.shape[0]


def line_up(parts):
    rows, columns = sum(p.shape[0] for p in parts), parts[0].shape[1]
    return pl.pallas_call(
        line_body,
        out_shape=vmem((rows, columns)),
        in_specs=[VMEM_SPEC] * len(parts),
        out_specs=VMEM_SPEC,
        compiler_params=limit(),
        name="line_up",
    )(*parts)


def half_body(first, whole, out):
    out[...] = whole[first : first + out.shape[0]]


def half_of(whole, upper):
    rows, columns = whole.shape
    return pl.pallas_call(
        functools.partial(half_body, upper * (rows // 2)),
        out_shape=vmem((rows // 2, columns)),
        in_specs=[VMEM_SPEC],
        out_specs=VMEM_SPEC,
        compiler_params=limit(),
        name="half_of",
    )(whole)


def order_body(tokens, own_tokens, own_gain, other_gain, images_out, gain_out, order_out):
    core, y, x = lax.axis_index("c"), lax.axis_index("y"), lax.axis_index("x")
    width = order_out.shape[0]
    place = lax.broadcasted_iota(jnp.int32, (1, width), 1)
    half, row = place // (width // 2), place % (width // 2)
    piece, share, element = row // 64, row % 64 // 16, row % 16
    rise = jnp.where(piece % 2 == 1, -((piece + 1) // 2), piece // 2)
    along = jnp.where(share <= 1, -share, share - 1)
    at = ((y + rise + 8) % 8 * 4 + (x + along + 4) % 4) * 2 + (core + half) % 2
    feature = at * 16 + element
    one_hot = lax.broadcasted_iota(jnp.int32, (width, width), 0) == feature
    order_out[...] = one_hot.astype(jnp.float32).astype(jnp.bfloat16)
    order = order_out[...]
    for i in range(images_out.shape[0]):
        mine = jnp.where(core == 0, own_tokens[i], tokens[i])
        images_out[i] = dot(mine, order).astype(jnp.bfloat16)
    rest = jnp.where(core == lax.axis_index("zl"), own_gain[...], other_gain[...])
    gain = jnp.zeros_like(rest)
    for _ in range(3):
        high = rest.astype(jnp.bfloat16)
        rest = rest - high.astype(jnp.float32)
        gain = gain + dot(jnp.broadcast_to(high, (8, width)), order)[:1]
    gain_out[...] = gain


def in_order(tokens, own_tokens, own_gain, other_gain):
    width = tokens.shape[-1]
    return pl.pallas_call(
        order_body,
        out_shape=(vmem(tokens.shape), vmem(own_gain.shape, jnp.float32), vmem((width, width))),
        in_specs=[VMEM_SPEC] * 4,
        out_specs=(VMEM_SPEC,) * 3,
        compiler_params=limit(12),
        cost_estimate=cost(1 << 26, 1 << 20),
        name="in_order",
    )(tokens, own_tokens, own_gain, other_gain)


def assemble_body(first, aliased, *refs):
    pieces, out = refs[int(aliased) : -1], refs[-1]
    for at, piece in zip(first, pieces, strict=True):
        out[at : at + piece.shape[0]] = piece[...]


def assemble(base, first, pieces):
    columns = pieces[0].shape[1]
    given = [] if base is None else [base]
    return pl.pallas_call(
        functools.partial(assemble_body, first, base is not None),
        out_shape=vmem((1024, columns)),
        in_specs=[VMEM_SPEC] * (len(given) + len(pieces)),
        out_specs=VMEM_SPEC,
        input_output_aliases={0: 0} if given else {},
        cost_estimate=cost(1 << 24, 1 << 20),
        compiler_params=limit(),
        name="assemble",
    )(*given, *pieces)


def core_swap(a):
    return lax.ppermute(a, "c", [(0, 1), (1, 0)])


def gathered(packed, gain, images):
    def moves(d):
        cells = [(c, x, z) for c in range(2) for x in range(4) for z in range(2)]
        return [(8 * c + 2 * x + z, 8 * z + 2 * ((x + d) % 4) + c) for c, x, z in cells]

    def up_ring(a):
        return lax.ppermute(a, "y", [(j, (j + 1) % 8) for j in range(8)])

    def down_ring(a):
        return lax.ppermute(a, "y", [(j, (j - 1) % 8) for j in range(8)])

    def to_pair(a):
        return lax.ppermute(a, ("c", "zl"), [(3, 2)])

    line = line_up([lax.ppermute(packed, ("c", "x", "zl"), moves(d)) for d in (0, 1, -1, 2)])
    up_1 = up_ring(line)
    down_1 = down_ring(line)
    beside = (core_swap(gain), to_pair(images))
    down_1, beside = lax.optimization_barrier((down_1, beside))
    up_2 = up_ring(up_1)
    down_2 = down_ring(down_1)
    ordered = in_order(beside[1], images, gain, beside[0])
    first = line_up([line, up_1, down_1, up_2])
    down_2, ordered = lax.optimization_barrier((down_2, ordered))
    up_3 = up_ring(up_2)
    down_3 = down_ring(down_2)
    other_first = core_swap(first)
    down_3, other_first = lax.optimization_barrier((down_3, other_first))
    up_4 = up_ring(half_of(up_3, 0))
    down_4 = down_ring(half_of(down_3, 1))
    second = line_up([down_2, up_3, down_3, up_4, down_4])
    other_second = core_swap(second)
    half, quarter = 512, 256
    base = assemble(None, (0, quarter, half), (first, second, other_first))
    return assemble(base, (half + quarter,), (other_second,)), ordered


def rows_body(*refs):
    order, streams, out, rows = refs[0], refs[1:-2], refs[-2], refs[-1]
    rows[...] = jnp.zeros_like(rows)
    for i, stream in enumerate(streams):
        rows[i : i + 1] = stream[0:1].astype(jnp.float32)
    out[...] = dot_t(rows[...].astype(jnp.bfloat16), order[...]).astype(jnp.bfloat16)


def class_rows(order, streams):
    width = streams[0].shape[1]
    return pl.pallas_call(
        rows_body,
        out_shape=vmem((8, width)),
        in_specs=[VMEM_SPEC] * (1 + len(streams)),
        out_specs=VMEM_SPEC,
        scratch_shapes=[vmem((8, width), jnp.float32)],
        compiler_params=limit(),
        name="class_rows",
    )(order, *streams)


def sum_body(*refs):
    total = refs[0][...]
    for ref in refs[1:-1]:
        total = total + ref[...]
    refs[-1][...] = total


def one_of(parts):
    return pl.pallas_call(
        sum_body,
        out_shape=vmem(parts[0].shape),
        in_specs=[VMEM_SPEC] * len(parts),
        out_specs=VMEM_SPEC,
        compiler_params=limit(),
        name="one_of",
    )(*parts)


def final_body(mine, other, gain_ref, head_ref, mean_ref, variance_ref, normed):
    here = lax.axis_index("c") == lax.axis_index("zl")
    rows = jnp.where(here, mine[...], other[...]).astype(jnp.float32)
    streams = 1 + TANGENTS
    gain = gain_ref[...]
    normed[...] = jnp.zeros_like(normed)
    for image in range(mean_ref.shape[0]):
        at = image * streams
        x = rows[at : at + 1]
        c = x - row_mean(x)
        r = lax.rsqrt(row_mean(c * c) + epsilon)
        normed[at : at + 1] = c * r * gain
        for j in range(1, streams):
            t = rows[at + j : at + j + 1]
            dc = t - row_mean(t)
            dr = -(r * r * r) * row_mean(c * dc)
            normed[at + j : at + j + 1] = (dc * r + c * dr) * gain
    logits = dot(normed[...].astype(jnp.bfloat16), head_ref[...])
    for image in range(mean_ref.shape[0]):
        at = image * streams
        mean_ref[image] = logits[at : at + 1]
        tangents = [logits[at + j : at + j + 1] for j in range(1, streams)]
        variance_ref[image] = sum(t * t for t in tangents)


def final_logits(mine, other, gain, head, micro):
    shape = jax.ShapeDtypeStruct((micro, 1, head.shape[1]), jnp.float32)
    return pl.pallas_call(
        final_body,
        out_shape=(shape, shape),
        in_specs=[VMEM_SPEC] * 4,
        out_specs=(VMEM_SPEC,) * 2,
        scratch_shapes=[vmem(mine.shape, jnp.float32)],
        compiler_params=limit(),
        name="final_logits",
    )(mine, other, gain, head)


def shards(tokens, w_qkv, w_output, tangent_value, tangent_output, layer_gain, final_gain, head):
    micro, _, length, width = tokens.shape
    images = tokens.reshape(micro, length, width)
    packed = pack(w_qkv, tangent_value, w_output, tangent_output)
    weights, (images, gain, order) = gathered(packed, layer_gain, images)

    stages = 8
    streams = (None,) * (1 + TANGENTS)
    last = []
    for step in range(stages + micro - 1):
        route = [(s, s + 1) for s in range(stages - 1) if 0 <= step - s < micro]
        out, normed, qkv, probs, attended = primal_layer(step, images, streams[0], gain, weights)
        results, moved = [out], []
        if route:
            moved.append(lax.ppermute(out, ("zh", "zl"), route))
        saved = (qkv, probs, *shared_layer(step, weights, normed, attended))
        for which in range(TANGENTS):
            out = tangent_layer(
                which, step, images, streams[0], streams[1 + which], gain, weights, saved
            )
            results.append(out)
            if route:
                moved.append(lax.ppermute(out, ("zh", "zl"), route))
        streams = tuple(moved)
        if step >= stages - 1:
            last += results
    rows = class_rows(order, last)
    sent = [
        lax.ppermute(rows, ("zh", "c", "zl"), [(13, 4 * i), (15, 4 * i + 3)]) for i in range(4)
    ]
    mine = one_of(sent)
    return final_logits(mine, core_swap(mine), final_gain[None], head, micro)


def solution(mesh):
    sizes = (4, 2, 8, 4, 2)
    split = Mesh(mesh.devices.reshape(sizes), ("zh", "c", "y", "x", "zl"))
    section, dp = ("zh", "c"), ("y", "x", "zl")
    return jax.shard_map(
        shards,
        mesh=split,
        in_specs=(
            P(None, dp, None, None),
            P(section, dp, None),
            P(section, None, dp),
            P(section, None, dp, None),
            P(section, None, None, dp),
            P(section, None),
            P(),
            P(None, section),
        ),
        out_specs=(P(None, dp, section), P(None, dp, section)),
        check_vma=False,
    )
```

```python
import functools

import jax
import jax.numpy as jnp
from jax import lax
from jax.experimental import pallas as pl
from jax.experimental.pallas import tpu as pltpu
from jax.sharding import Mesh
from jax.sharding import PartitionSpec as P

HEADS = 8
HEAD = 64
TANGENTS = 2
HD = 512
PAIR = 2 * HEAD
PAIRS = HEADS // 2
SCALE = HEAD ** (-0.5)

epsilon = 1e-06

QKV = slice(0, 3 * HD)
TV = (slice(3 * HD, 4 * HD), slice(4 * HD, 5 * HD))
WO = slice(5 * HD, 6 * HD)
TO = (slice(6 * HD, 7 * HD), slice(7 * HD, 8 * HD))


VMEM_SPEC = pl.BlockSpec(memory_space=pltpu.VMEM)
HBM_SPEC = pl.BlockSpec(memory_space=pltpu.HBM)


def dot(left, right):
    return jnp.dot(left, right, preferred_element_type=jnp.float32)


def dot_t(left, right):
    return lax.dot_general(
        left, right, (((1,), (1,)), ((), ())), preferred_element_type=jnp.float32
    )


def row_mean(a):
    return jnp.sum(a, -1, keepdims=True) * (1.0 / a.shape[-1])


def head_masks(rows):
    lane = lax.broadcasted_iota(jnp.int32, (rows, PAIR), 1)
    return lane < HEAD, lane >= HEAD


def part(ref, which, pair):
    at = which * HD + pair * PAIR
    return ref[:, at : at + PAIR]


def masked(a, mask):
    return jnp.where(mask, a, jnp.zeros_like(a))


def plane_of_this():
    return 2 * lax.axis_index("zh") + lax.axis_index("zl")


def working(step, plane):
    return (step - plane >= 0) & (step - plane < 2)


def entering(step, plane, images, stream, t_stream=None):
    if step < 2:
        x = images[step].astype(jnp.float32)
        t = jnp.zeros_like(x)
        if step == 1:
            x = jnp.where(plane == 0, x, stream[...].astype(jnp.float32))
            if t_stream is not None:
                t = jnp.where(plane == 0, t, t_stream[...].astype(jnp.float32))
        return x, t
    return (
        stream[...].astype(jnp.float32),
        None if t_stream is None else t_stream[...].astype(jnp.float32),
    )


def primal_body(step, *refs):
    gain_ref, w_ref, out_ref, n_ref, qkv_ref, p_ref, att_ref = refs[-7:]
    images, streams = refs[0] if step < 2 else None, refs[1 if step < 2 else 0 : -7]
    plane = plane_of_this()

    @pl.when(working(step, plane))
    def _():
        x, _ = entering(step, plane, images, *streams[:1] or (None,))
        gain = gain_ref[...]
        c = x - row_mean(x)
        r = lax.rsqrt(row_mean(c * c) + epsilon)
        n = (c * r * gain).astype(jnp.bfloat16)
        n_ref[...] = n
        qkv_ref[...] = dot(n, w_ref[:, QKV]).astype(jnp.bfloat16)
        masks = head_masks(x.shape[0])
        for pair in range(PAIRS):
            q, k, v = (part(qkv_ref, i, pair) for i in range(3))
            total = None
            for half in range(2):
                s = dot_t(masked(q, masks[half]), k) * SCALE
                e = jnp.exp(s - jnp.max(s, -1, keepdims=True))
                p = e / jnp.sum(e, -1, keepdims=True)
                p_ref[2 * pair + half] = p
                a = dot(p.astype(jnp.bfloat16), masked(v, masks[half]))
                total = a if total is None else total + a
            att_ref[:, pair * PAIR : (pair + 1) * PAIR] = total.astype(jnp.bfloat16)
        out_ref[...] = (x + dot_t(att_ref[...], w_ref[:, WO])).astype(jnp.bfloat16)


def shared_body(step, w_ref, n_ref, att_ref, values_ref, outs_ref):
    @pl.when(working(step, plane_of_this()))
    def _():
        for which in range(TANGENTS):
            values_ref[which] = dot(n_ref[...], w_ref[:, TV[which]])
            outs_ref[which] = dot_t(att_ref[...], w_ref[:, TO[which]])


def tangent_body(which, step, *refs):
    gain_ref, w_ref, qkv_ref, p_ref, values_ref, outs_ref, out_ref, mine, joined = refs[-9:]
    images, streams = refs[0] if step < 2 else None, refs[1 if step < 2 else 0 : -9]
    plane = plane_of_this()

    @pl.when(working(step, plane))
    def _():
        x, t = entering(step, plane, images, *(streams or (None, None)))
        gain = gain_ref[...]
        c = x - row_mean(x)
        r = lax.rsqrt(row_mean(c * c) + epsilon)
        dc = t - row_mean(t)
        dr = -(r * r * r) * row_mean(c * dc)
        dn = ((dc * r + c * dr) * gain).astype(jnp.bfloat16)
        mine[:, : 2 * HD] = dot(dn, w_ref[:, : 2 * HD]).astype(jnp.bfloat16)
        values = dot(dn, w_ref[:, 2 * HD : 3 * HD]) + values_ref[which]
        mine[:, 2 * HD :] = values.astype(jnp.bfloat16)
        masks = head_masks(x.shape[0])
        for pair in range(PAIRS):
            q0, k0, v0 = (part(qkv_ref, i, pair) for i in range(3))
            q1, k1, v1 = (part(mine, i, pair) for i in range(3))
            total = None
            for half in range(2):
                m = masks[half]
                ds = (dot_t(masked(q1, m), k0) + dot_t(masked(q0, m), k1)) * SCALE
                p = p_ref[2 * pair + half]
                dp = p * (ds - jnp.sum(p * ds, -1, keepdims=True))
                a = dot(dp.astype(jnp.bfloat16), masked(v0, m)) + dot(
                    p.astype(jnp.bfloat16), masked(v1, m)
                )
                total = a if total is None else total + a
            joined[:, pair * PAIR : (pair + 1) * PAIR] = total.astype(jnp.bfloat16)
        moved = dot_t(joined[...], w_ref[:, WO]) + outs_ref[which]
        out_ref[...] = (t + moved).astype(jnp.bfloat16)


def cost(flops, bytes_accessed):
    return pl.CostEstimate(flops=flops, bytes_accessed=bytes_accessed, transcendentals=0)


def vmem(shape, dtype=jnp.bfloat16):
    return pltpu.VMEM(shape, dtype)


def in_hbm(a):
    return pltpu.with_memory_space_constraint(a, pltpu.HBM)


def limit(mib=4):
    return pltpu.CompilerParams(vmem_limit_bytes=mib << 20)


def primal_layer(step, images, x, gain, weights):
    tokens, width = images.shape[1:]
    bf16 = jnp.bfloat16
    given = (*((images,) if step < 2 else ()), *((x,) if step else ()), gain, weights)
    return pl.pallas_call(
        functools.partial(primal_body, step),
        out_shape=(
            jax.ShapeDtypeStruct((tokens, width), bf16),
            jax.ShapeDtypeStruct((tokens, width), bf16),
            jax.ShapeDtypeStruct((tokens, 3 * HD), bf16),
            jax.ShapeDtypeStruct((HEADS, tokens, tokens), jnp.float32),
            jax.ShapeDtypeStruct((tokens, HD), bf16),
        ),
        in_specs=[VMEM_SPEC] * len(given),
        out_specs=(VMEM_SPEC,) * 5,
        cost_estimate=cost(2 * tokens * width * 4 * HD, 1 << 20),
        compiler_params=limit(12),
        name="primal_layer",
    )(*given)


def shared_layer(step, weights, normed, attended):
    tokens, width = normed.shape
    return pl.pallas_call(
        functools.partial(shared_body, step),
        out_shape=(
            jax.ShapeDtypeStruct((TANGENTS, tokens, HD), jnp.float32),
            jax.ShapeDtypeStruct((TANGENTS, tokens, width), jnp.float32),
        ),
        in_specs=[VMEM_SPEC] * 3,
        out_specs=(VMEM_SPEC,) * 2,
        cost_estimate=cost(2 * tokens * width * 4 * HD, 1 << 20),
        compiler_params=limit(12),
        name="shared_layer",
    )(weights, normed, attended)


def tangent_layer(which, step, images, x, t, gain, weights, saved):
    tokens, width = images.shape[1:]
    given = (*((images,) if step < 2 else ()), *((x, t) if step else ()), gain, weights, *saved)
    return pl.pallas_call(
        functools.partial(tangent_body, which, step),
        out_shape=jax.ShapeDtypeStruct((tokens, width), jnp.bfloat16),
        in_specs=[VMEM_SPEC] * len(given),
        out_specs=VMEM_SPEC,
        scratch_shapes=[vmem((tokens, 3 * HD)), vmem((tokens, HD))],
        cost_estimate=cost(2 * tokens * width * 4 * HD, 1 << 20),
        compiler_params=limit(12),
    )(*given)


def copied(pairs, sems):
    copies = [pltpu.make_async_copy(a, b, sems.at[i]) for i, (a, b) in enumerate(pairs)]
    for copy in copies:
        copy.start()
    for copy in copies:
        copy.wait()


def pack_body(qkv, value, output, tangent_output, out, sems):
    pairs = [(qkv.at[0], out.at[:, QKV]), (output.at[0], out.at[:, WO])]
    for which in range(TANGENTS):
        pairs.append((value.at[0, which], out.at[:, TV[which]]))
        pairs.append((tangent_output.at[0, which], out.at[:, TO[which]]))
    copied(pairs, sems)


def pack(w_qkv, tangent_value, w_output, tangent_output):
    shares = (w_qkv, tangent_value, w_output.swapaxes(1, 2), tangent_output.swapaxes(2, 3))
    return pl.pallas_call(
        pack_body,
        out_shape=vmem((w_qkv.shape[1], 8 * HD)),
        in_specs=[HBM_SPEC] * 4,
        out_specs=VMEM_SPEC,
        scratch_shapes=[pltpu.SemaphoreType.DMA((2 + 2 * TANGENTS,))],
        compiler_params=limit(),
        name="pack",
    )(*map(in_hbm, shares))


def line_body(*refs):
    parts, out = refs[:-1], refs[-1]
    at = 0
    for part in parts:
        out[at : at + part.shape[0]] = part[...]
        at += part.shape[0]


def line_up(parts):
    rows, columns = sum(p.shape[0] for p in parts), parts[0].shape[1]
    return pl.pallas_call(
        line_body,
        out_shape=vmem((rows, columns)),
        in_specs=[VMEM_SPEC] * len(parts),
        out_specs=VMEM_SPEC,
        compiler_params=limit(),
        name="line_up",
    )(*parts)


def order_body(tokens, own_tokens, own_gain, other_gain, images_out, gain_out, order_out):
    core, y, x = lax.axis_index("c"), lax.axis_index("y"), lax.axis_index("x")
    width = order_out.shape[0]
    place = lax.broadcasted_iota(jnp.int32, (1, width), 1)
    half, row = place // (width // 2), place % (width // 2)
    piece, share, element = row // 64, row % 64 // 16, row % 16
    rise = jnp.where(piece % 2 == 1, -((piece + 1) // 2), piece // 2)
    along = jnp.where(share <= 1, -share, share - 1)
    at = ((y + rise + 8) % 8 * 4 + (x + along + 4) % 4) * 2 + (core + half) % 2
    feature = at * 16 + element
    one_hot = lax.broadcasted_iota(jnp.int32, (width, width), 0) == feature
    order_out[...] = one_hot.astype(jnp.float32).astype(jnp.bfloat16)
    order = order_out[...]
    for i in range(images_out.shape[0]):
        mine = jnp.where(core == 0, own_tokens[i], tokens[i])
        images_out[i] = dot(mine, order).astype(jnp.bfloat16)
    rest = jnp.where(core == lax.axis_index("zl"), own_gain[...], other_gain[...])
    gain = jnp.zeros_like(rest)
    for _ in range(3):
        high = rest.astype(jnp.bfloat16)
        rest = rest - high.astype(jnp.float32)
        gain = gain + dot(jnp.broadcast_to(high, (8, width)), order)[:1]
    gain_out[...] = gain


def in_order(tokens, own_tokens, own_gain, other_gain):
    width = tokens.shape[-1]
    return pl.pallas_call(
        order_body,
        out_shape=(vmem(tokens.shape), vmem(own_gain.shape, jnp.float32), vmem((width, width))),
        in_specs=[VMEM_SPEC] * 4,
        out_specs=(VMEM_SPEC,) * 3,
        compiler_params=limit(12),
        cost_estimate=cost(1 << 26, 1 << 20),
        name="in_order",
    )(tokens, own_tokens, own_gain, other_gain)


def assemble_body(first, aliased, *refs):
    pieces, out = refs[int(aliased) : -1], refs[-1]
    for at, piece in zip(first, pieces, strict=True):
        out[at : at + piece.shape[0]] = piece[...]


def assemble(base, first, pieces):
    columns = pieces[0].shape[1]
    given = [] if base is None else [base]
    return pl.pallas_call(
        functools.partial(assemble_body, first, base is not None),
        out_shape=vmem((1024, columns)),
        in_specs=[VMEM_SPEC] * (len(given) + len(pieces)),
        out_specs=VMEM_SPEC,
        input_output_aliases={0: 0} if given else {},
        cost_estimate=cost(1 << 24, 1 << 20),
        compiler_params=limit(),
        name="assemble",
    )(*given, *pieces)


def core_swap(a):
    return lax.ppermute(a, "c", [(0, 1), (1, 0)])


def gathered(packed, gain, images):
    def moves(d):
        cells = [(c, x, z) for c in range(2) for x in range(4) for z in range(2)]
        return [(8 * c + 2 * x + z, 8 * z + 2 * ((x + d) % 4) + c) for c, x, z in cells]

    def up_ring(a):
        return lax.ppermute(a, "y", [(j, (j + 1) % 8) for j in range(8)])

    def down_ring(a):
        return lax.ppermute(a, "y", [(j, (j - 1) % 8) for j in range(8)])

    def to_pair(a):
        return lax.ppermute(a, ("c", "zl"), [(3, 2)])

    shares = [lax.ppermute(packed, ("c", "x", "zl"), moves(d)) for d in (0, 1, -1, 2)]
    line = [line_up(shares[:2]), line_up(shares[2:])]

    def ring(way, halves):
        move = up_ring if way == "up" else down_ring
        return [move(h) for h in halves]

    up_1, down_1 = ring("up", line), ring("down", line)
    beside = (core_swap(gain), to_pair(images))
    down_1[1], beside = lax.optimization_barrier((down_1[1], beside))
    up_2, down_2 = ring("up", up_1), ring("down", down_1)
    ordered = in_order(beside[1], images, gain, beside[0])
    first = line_up([*line, *up_1, *down_1, *up_2])
    down_2[1], ordered = lax.optimization_barrier((down_2[1], ordered))
    up_3, down_3 = ring("up", up_2), ring("down", down_2)
    other_first = core_swap(first)
    down_3[1], other_first = lax.optimization_barrier((down_3[1], other_first))
    up_4 = up_ring(up_3[0])
    down_4 = down_ring(down_3[1])
    second = line_up([*down_2, *up_3, *down_3, up_4, down_4])
    other_second = core_swap(second)
    half, quarter = 512, 256
    base = assemble(None, (0, quarter, half), (first, second, other_first))
    return assemble(base, (half + quarter,), (other_second,)), ordered


def rows_body(*refs):
    order, streams, out, rows = refs[0], refs[1:-2], refs[-2], refs[-1]
    rows[...] = jnp.zeros_like(rows)
    for i, stream in enumerate(streams):
        rows[i : i + 1] = stream[0:1].astype(jnp.float32)
    out[...] = dot_t(rows[...].astype(jnp.bfloat16), order[...]).astype(jnp.bfloat16)


def class_rows(order, streams):
    width = streams[0].shape[1]
    return pl.pallas_call(
        rows_body,
        out_shape=vmem((8, width)),
        in_specs=[VMEM_SPEC] * (1 + len(streams)),
        out_specs=VMEM_SPEC,
        scratch_shapes=[vmem((8, width), jnp.float32)],
        compiler_params=limit(),
        name="class_rows",
    )(order, *streams)


def sum_body(*refs):
    total = refs[0][...]
    for ref in refs[1:-1]:
        total = total + ref[...]
    refs[-1][...] = total


def one_of(parts):
    return pl.pallas_call(
        sum_body,
        out_shape=vmem(parts[0].shape),
        in_specs=[VMEM_SPEC] * len(parts),
        out_specs=VMEM_SPEC,
        compiler_params=limit(),
        name="one_of",
    )(*parts)


def final_body(mine, other, gain_ref, head_ref, mean_ref, variance_ref, normed):
    here = lax.axis_index("c") == lax.axis_index("zl")
    rows = jnp.where(here, mine[...], other[...]).astype(jnp.float32)
    streams = 1 + TANGENTS
    gain = gain_ref[...]
    normed[...] = jnp.zeros_like(normed)
    for image in range(mean_ref.shape[0]):
        at = image * streams
        x = rows[at : at + 1]
        c = x - row_mean(x)
        r = lax.rsqrt(row_mean(c * c) + epsilon)
        normed[at : at + 1] = c * r * gain
        for j in range(1, streams):
            t = rows[at + j : at + j + 1]
            dc = t - row_mean(t)
            dr = -(r * r * r) * row_mean(c * dc)
            normed[at + j : at + j + 1] = (dc * r + c * dr) * gain
    logits = dot(normed[...].astype(jnp.bfloat16), head_ref[...])
    for image in range(mean_ref.shape[0]):
        at = image * streams
        mean_ref[image] = logits[at : at + 1]
        tangents = [logits[at + j : at + j + 1] for j in range(1, streams)]
        variance_ref[image] = sum(t * t for t in tangents)


def final_logits(mine, other, gain, head, micro):
    shape = jax.ShapeDtypeStruct((micro, 1, head.shape[1]), jnp.float32)
    return pl.pallas_call(
        final_body,
        out_shape=(shape, shape),
        in_specs=[VMEM_SPEC] * 4,
        out_specs=(VMEM_SPEC,) * 2,
        scratch_shapes=[vmem(mine.shape, jnp.float32)],
        compiler_params=limit(),
        name="final_logits",
    )(mine, other, gain, head)


def shards(tokens, w_qkv, w_output, tangent_value, tangent_output, layer_gain, final_gain, head):
    micro, _, length, width = tokens.shape
    images = tokens.reshape(micro, length, width)
    packed = pack(w_qkv, tangent_value, w_output, tangent_output)
    weights, (images, gain, order) = gathered(packed, layer_gain, images)

    stages = 8
    streams = (None,) * (1 + TANGENTS)
    last = []
    for step in range(stages + micro - 1):
        route = [(s, s + 1) for s in range(stages - 1) if 0 <= step - s < micro]
        out, normed, qkv, probs, attended = primal_layer(step, images, streams[0], gain, weights)
        results, moved = [out], []
        if route:
            moved.append(lax.ppermute(out, ("zh", "zl"), route))
        saved = (qkv, probs, *shared_layer(step, weights, normed, attended))
        for which in range(TANGENTS):
            out = tangent_layer(
                which, step, images, streams[0], streams[1 + which], gain, weights, saved
            )
            results.append(out)
            if route:
                moved.append(lax.ppermute(out, ("zh", "zl"), route))
        streams = tuple(moved)
        if step >= stages - 1:
            last += results
    rows = class_rows(order, last)
    sent = [
        lax.ppermute(rows, ("zh", "c", "zl"), [(13, 4 * i), (15, 4 * i + 3)]) for i in range(4)
    ]
    mine = one_of(sent)
    return final_logits(mine, core_swap(mine), final_gain[None], head, micro)


def solution(mesh):
    sizes = (4, 2, 8, 4, 2)
    split = Mesh(mesh.devices.reshape(sizes), ("zh", "c", "y", "x", "zl"))
    section, dp = ("zh", "c"), ("y", "x", "zl")
    return jax.shard_map(
        shards,
        mesh=split,
        in_specs=(
            P(None, dp, None, None),
            P(section, dp, None),
            P(section, None, dp),
            P(section, None, dp, None),
            P(section, None, None, dp),
            P(section, None),
            P(),
            P(None, section),
        ),
        out_specs=(P(None, dp, section), P(None, dp, section)),
        check_vma=False,
    )
```

```python
import functools

import jax
import jax.numpy as jnp
from jax import lax
from jax.experimental import pallas as pl
from jax.experimental.pallas import tpu as pltpu
from jax.sharding import Mesh
from jax.sharding import PartitionSpec as P

HEADS = 8
HEAD = 64
TANGENTS = 2
HD = 512
PAIR = 2 * HEAD
PAIRS = HEADS // 2
SCALE = HEAD ** (-0.5)

epsilon = 1e-06

QKV = slice(0, 3 * HD)
TV = (slice(3 * HD, 4 * HD), slice(4 * HD, 5 * HD))
WO = slice(5 * HD, 6 * HD)
TO = (slice(6 * HD, 7 * HD), slice(7 * HD, 8 * HD))


VMEM_SPEC = pl.BlockSpec(memory_space=pltpu.VMEM)
HBM_SPEC = pl.BlockSpec(memory_space=pltpu.HBM)


def dot(left, right):
    return jnp.dot(left, right, preferred_element_type=jnp.float32)


def dot_t(left, right):
    return lax.dot_general(
        left, right, (((1,), (1,)), ((), ())), preferred_element_type=jnp.float32
    )


def row_mean(a):
    return jnp.sum(a, -1, keepdims=True) * (1.0 / a.shape[-1])


def head_masks(rows):
    lane = lax.broadcasted_iota(jnp.int32, (rows, PAIR), 1)
    return lane < HEAD, lane >= HEAD


def part(ref, which, pair):
    at = which * HD + pair * PAIR
    return ref[:, at : at + PAIR]


def masked(a, mask):
    return jnp.where(mask, a, jnp.zeros_like(a))


def plane_of_this():
    return 2 * lax.axis_index("zh") + lax.axis_index("zl")


def working(step, plane):
    return (step - plane >= 0) & (step - plane < 2)


def entering(step, plane, images, stream, t_stream=None):
    if step < 2:
        x = images[step].astype(jnp.float32)
        t = jnp.zeros_like(x)
        if step == 1:
            x = jnp.where(plane == 0, x, stream[...].astype(jnp.float32))
            if t_stream is not None:
                t = jnp.where(plane == 0, t, t_stream[...].astype(jnp.float32))
        return x, t
    return (
        stream[...].astype(jnp.float32),
        None if t_stream is None else t_stream[...].astype(jnp.float32),
    )


def primal_body(step, *refs):
    gain_ref, w_ref, out_ref, n_ref, qkv_ref, p_ref, att_ref = refs[-7:]
    images, streams = refs[0] if step < 2 else None, refs[1 if step < 2 else 0 : -7]
    plane = plane_of_this()

    @pl.when(working(step, plane))
    def _():
        x, _ = entering(step, plane, images, *streams[:1] or (None,))
        gain = gain_ref[...]
        c = x - row_mean(x)
        r = lax.rsqrt(row_mean(c * c) + epsilon)
        n = (c * r * gain).astype(jnp.bfloat16)
        n_ref[...] = n
        qkv_ref[...] = dot(n, w_ref[:, QKV]).astype(jnp.bfloat16)
        masks = head_masks(x.shape[0])
        for pair in range(PAIRS):
            q, k, v = (part(qkv_ref, i, pair) for i in range(3))
            total = None
            for half in range(2):
                s = dot_t(masked(q, masks[half]), k) * SCALE
                e = jnp.exp(s - jnp.max(s, -1, keepdims=True))
                p = e / jnp.sum(e, -1, keepdims=True)
                p_ref[2 * pair + half] = p
                a = dot(p.astype(jnp.bfloat16), masked(v, masks[half]))
                total = a if total is None else total + a
            att_ref[:, pair * PAIR : (pair + 1) * PAIR] = total.astype(jnp.bfloat16)
        out_ref[...] = (x + dot_t(att_ref[...], w_ref[:, WO])).astype(jnp.bfloat16)


def shared_body(step, w_ref, n_ref, att_ref, values_ref, outs_ref):
    @pl.when(working(step, plane_of_this()))
    def _():
        for which in range(TANGENTS):
            values_ref[which] = dot(n_ref[...], w_ref[:, TV[which]])
            outs_ref[which] = dot_t(att_ref[...], w_ref[:, TO[which]])


def tangent_body(which, step, *refs):
    gain_ref, w_ref, qkv_ref, p_ref, values_ref, outs_ref, out_ref, mine, joined = refs[-9:]
    images, streams = refs[0] if step < 2 else None, refs[1 if step < 2 else 0 : -9]
    plane = plane_of_this()

    @pl.when(working(step, plane))
    def _():
        x, t = entering(step, plane, images, *(streams or (None, None)))
        gain = gain_ref[...]
        c = x - row_mean(x)
        r = lax.rsqrt(row_mean(c * c) + epsilon)
        dc = t - row_mean(t)
        dr = -(r * r * r) * row_mean(c * dc)
        dn = ((dc * r + c * dr) * gain).astype(jnp.bfloat16)
        mine[:, : 2 * HD] = dot(dn, w_ref[:, : 2 * HD]).astype(jnp.bfloat16)
        values = dot(dn, w_ref[:, 2 * HD : 3 * HD]) + values_ref[which]
        mine[:, 2 * HD :] = values.astype(jnp.bfloat16)
        masks = head_masks(x.shape[0])
        for pair in range(PAIRS):
            q0, k0, v0 = (part(qkv_ref, i, pair) for i in range(3))
            q1, k1, v1 = (part(mine, i, pair) for i in range(3))
            total = None
            for half in range(2):
                m = masks[half]
                ds = (dot_t(masked(q1, m), k0) + dot_t(masked(q0, m), k1)) * SCALE
                p = p_ref[2 * pair + half]
                dp = p * (ds - jnp.sum(p * ds, -1, keepdims=True))
                a = dot(dp.astype(jnp.bfloat16), masked(v0, m)) + dot(
                    p.astype(jnp.bfloat16), masked(v1, m)
                )
                total = a if total is None else total + a
            joined[:, pair * PAIR : (pair + 1) * PAIR] = total.astype(jnp.bfloat16)
        moved = dot_t(joined[...], w_ref[:, WO]) + outs_ref[which]
        out_ref[...] = (t + moved).astype(jnp.bfloat16)


def cost(flops, bytes_accessed):
    return pl.CostEstimate(flops=flops, bytes_accessed=bytes_accessed, transcendentals=0)


def vmem(shape, dtype=jnp.bfloat16):
    return pltpu.VMEM(shape, dtype)


def in_hbm(a):
    return pltpu.with_memory_space_constraint(a, pltpu.HBM)


def limit(mib=4):
    return pltpu.CompilerParams(vmem_limit_bytes=mib << 20)


def primal_layer(step, images, x, gain, weights):
    tokens, width = images.shape[1:]
    bf16 = jnp.bfloat16
    given = (*((images,) if step < 2 else ()), *((x,) if step else ()), gain, weights)
    return pl.pallas_call(
        functools.partial(primal_body, step),
        out_shape=(
            jax.ShapeDtypeStruct((tokens, width), bf16),
            jax.ShapeDtypeStruct((tokens, width), bf16),
            jax.ShapeDtypeStruct((tokens, 3 * HD), bf16),
            jax.ShapeDtypeStruct((HEADS, tokens, tokens), jnp.float32),
            jax.ShapeDtypeStruct((tokens, HD), bf16),
        ),
        in_specs=[VMEM_SPEC] * len(given),
        out_specs=(VMEM_SPEC,) * 5,
        cost_estimate=cost(2 * tokens * width * 4 * HD, 1 << 20),
        compiler_params=limit(12),
        name="primal_layer",
    )(*given)


def shared_layer(step, weights, normed, attended):
    tokens, width = normed.shape
    return pl.pallas_call(
        functools.partial(shared_body, step),
        out_shape=(
            jax.ShapeDtypeStruct((TANGENTS, tokens, HD), jnp.float32),
            jax.ShapeDtypeStruct((TANGENTS, tokens, width), jnp.float32),
        ),
        in_specs=[VMEM_SPEC] * 3,
        out_specs=(VMEM_SPEC,) * 2,
        cost_estimate=cost(2 * tokens * width * 4 * HD, 1 << 20),
        compiler_params=limit(12),
        name="shared_layer",
    )(weights, normed, attended)


def tangent_layer(which, step, images, x, t, gain, weights, saved):
    tokens, width = images.shape[1:]
    given = (*((images,) if step < 2 else ()), *((x, t) if step else ()), gain, weights, *saved)
    return pl.pallas_call(
        functools.partial(tangent_body, which, step),
        out_shape=jax.ShapeDtypeStruct((tokens, width), jnp.bfloat16),
        in_specs=[VMEM_SPEC] * len(given),
        out_specs=VMEM_SPEC,
        scratch_shapes=[vmem((tokens, 3 * HD)), vmem((tokens, HD))],
        cost_estimate=cost(2 * tokens * width * 4 * HD, 1 << 20),
        compiler_params=limit(12),
    )(*given)


def copied(pairs, sems):
    copies = [pltpu.make_async_copy(a, b, sems.at[i]) for i, (a, b) in enumerate(pairs)]
    for copy in copies:
        copy.start()
    for copy in copies:
        copy.wait()


def pack_body(qkv, value, output, tangent_output, out, sems):
    pairs = [(qkv.at[0], out.at[:, QKV]), (output.at[0], out.at[:, WO])]
    for which in range(TANGENTS):
        pairs.append((value.at[0, which], out.at[:, TV[which]]))
        pairs.append((tangent_output.at[0, which], out.at[:, TO[which]]))
    copied(pairs, sems)


def pack(w_qkv, tangent_value, w_output, tangent_output):
    shares = (w_qkv, tangent_value, w_output.swapaxes(1, 2), tangent_output.swapaxes(2, 3))
    return pl.pallas_call(
        pack_body,
        out_shape=vmem((w_qkv.shape[1], 8 * HD)),
        in_specs=[HBM_SPEC] * 4,
        out_specs=VMEM_SPEC,
        scratch_shapes=[pltpu.SemaphoreType.DMA((2 + 2 * TANGENTS,))],
        compiler_params=limit(),
        name="pack",
    )(*map(in_hbm, shares))


def line_body(*refs):
    parts, out = refs[:-1], refs[-1]
    at = 0
    for part in parts:
        out[at : at + part.shape[0]] = part[...]
        at += part.shape[0]


def line_up(parts):
    rows, columns = sum(p.shape[0] for p in parts), parts[0].shape[1]
    return pl.pallas_call(
        line_body,
        out_shape=vmem((rows, columns)),
        in_specs=[VMEM_SPEC] * len(parts),
        out_specs=VMEM_SPEC,
        compiler_params=limit(),
        name="line_up",
    )(*parts)


def half_body(first, whole, out):
    out[...] = whole[first : first + out.shape[0]]


def half_of(whole, upper):
    rows, columns = whole.shape
    return pl.pallas_call(
        functools.partial(half_body, upper * (rows // 2)),
        out_shape=vmem((rows // 2, columns)),
        in_specs=[VMEM_SPEC],
        out_specs=VMEM_SPEC,
        compiler_params=limit(),
        name="half_of",
    )(whole)


def order_body(tokens, own_tokens, own_gain, other_gain, images_out, gain_out, order_out):
    core, y, x = lax.axis_index("c"), lax.axis_index("y"), lax.axis_index("x")
    width = order_out.shape[0]
    place = lax.broadcasted_iota(jnp.int32, (1, width), 1)
    half, row = place // (width // 2), place % (width // 2)
    piece, share, element = row // 64, row % 64 // 16, row % 16
    rise = jnp.where(piece % 2 == 1, -((piece + 1) // 2), piece // 2)
    along = jnp.where(share <= 1, -share, share - 1)
    at = ((y + rise + 8) % 8 * 4 + (x + along + 4) % 4) * 2 + (core + half) % 2
    feature = at * 16 + element
    one_hot = lax.broadcasted_iota(jnp.int32, (width, width), 0) == feature
    order_out[...] = one_hot.astype(jnp.float32).astype(jnp.bfloat16)
    order = order_out[...]
    for i in range(images_out.shape[0]):
        mine = jnp.where(core == 0, own_tokens[i], tokens[i])
        images_out[i] = dot(mine, order).astype(jnp.bfloat16)
    rest = jnp.where(core == lax.axis_index("zl"), own_gain[...], other_gain[...])
    gain = jnp.zeros_like(rest)
    for _ in range(3):
        high = rest.astype(jnp.bfloat16)
        rest = rest - high.astype(jnp.float32)
        gain = gain + dot(jnp.broadcast_to(high, (8, width)), order)[:1]
    gain_out[...] = gain


def in_order(tokens, own_tokens, own_gain, other_gain):
    width = tokens.shape[-1]
    return pl.pallas_call(
        order_body,
        out_shape=(vmem(tokens.shape), vmem(own_gain.shape, jnp.float32), vmem((width, width))),
        in_specs=[VMEM_SPEC] * 4,
        out_specs=(VMEM_SPEC,) * 3,
        compiler_params=limit(12),
        cost_estimate=cost(1 << 26, 1 << 20),
        name="in_order",
    )(tokens, own_tokens, own_gain, other_gain)


def assemble_body(first, aliased, *refs):
    pieces, out = refs[int(aliased) : -1], refs[-1]
    for at, piece in zip(first, pieces, strict=True):
        out[at : at + piece.shape[0]] = piece[...]


def assemble(base, first, pieces):
    columns = pieces[0].shape[1]
    given = [] if base is None else [base]
    return pl.pallas_call(
        functools.partial(assemble_body, first, base is not None),
        out_shape=vmem((1024, columns)),
        in_specs=[VMEM_SPEC] * (len(given) + len(pieces)),
        out_specs=VMEM_SPEC,
        input_output_aliases={0: 0} if given else {},
        cost_estimate=cost(1 << 24, 1 << 20),
        compiler_params=limit(),
        name="assemble",
    )(*given, *pieces)


def core_swap(a):
    return lax.ppermute(a, "c", [(0, 1), (1, 0)])


def gathered(packed, gain, images):
    def moves(d):
        cells = [(c, x, z) for c in range(2) for x in range(4) for z in range(2)]
        return [(8 * c + 2 * x + z, 8 * z + 2 * ((x + d) % 4) + c) for c, x, z in cells]

    def up_ring(a):
        return lax.ppermute(a, "y", [(j, (j + 1) % 8) for j in range(8)])

    def down_ring(a):
        return lax.ppermute(a, "y", [(j, (j - 1) % 8) for j in range(8)])

    def to_pair(a):
        return lax.ppermute(a, ("c", "zl"), [(3, 2)])

    line = line_up([lax.ppermute(packed, ("c", "x", "zl"), moves(d)) for d in (0, 1, -1, 2)])
    up_1 = up_ring(line)
    down_1 = down_ring(line)
    beside = (core_swap(gain), to_pair(images))
    up_2 = up_ring(up_1)
    early = line_up([line, up_1])
    down_1, early = lax.optimization_barrier((down_1, early))
    down_2 = down_ring(down_1)
    ordered = in_order(beside[1], images, gain, beside[0])
    up_2, ordered = lax.optimization_barrier((up_2, ordered))
    up_3 = up_ring(up_2)
    early = line_up([early, down_1, up_2])
    down_2, early = lax.optimization_barrier((down_2, early))
    down_3 = down_ring(down_2)
    first = line_up([early, down_2])
    other_first = core_swap(first)
    up_3, other_first = lax.optimization_barrier((up_3, other_first))
    up_4 = up_ring(half_of(up_3, 0))
    down_4 = down_ring(half_of(down_3, 1))
    second = line_up([up_3, down_3])
    other_second = core_swap(second)
    up_4, other_second = lax.optimization_barrier((up_4, other_second))
    third = line_up([up_4, down_4])
    other_third = core_swap(third)
    base = assemble(None, (0, 320, 448, 512, 832), (first, second, third, other_first, other_second))
    return assemble(base, (960,), (other_third,)), ordered


def rows_body(*refs):
    order, streams, out, rows = refs[0], refs[1:-2], refs[-2], refs[-1]
    rows[...] = jnp.zeros_like(rows)
    for i, stream in enumerate(streams):
        rows[i : i + 1] = stream[0:1].astype(jnp.float32)
    out[...] = dot_t(rows[...].astype(jnp.bfloat16), order[...]).astype(jnp.bfloat16)


def class_rows(order, streams):
    width = streams[0].shape[1]
    return pl.pallas_call(
        rows_body,
        out_shape=vmem((8, width)),
        in_specs=[VMEM_SPEC] * (1 + len(streams)),
        out_specs=VMEM_SPEC,
        scratch_shapes=[vmem((8, width), jnp.float32)],
        compiler_params=limit(),
        name="class_rows",
    )(order, *streams)


def sum_body(*refs):
    total = refs[0][...]
    for ref in refs[1:-1]:
        total = total + ref[...]
    refs[-1][...] = total


def one_of(parts):
    return pl.pallas_call(
        sum_body,
        out_shape=vmem(parts[0].shape),
        in_specs=[VMEM_SPEC] * len(parts),
        out_specs=VMEM_SPEC,
        compiler_params=limit(),
        name="one_of",
    )(*parts)


def final_body(mine, other, gain_ref, head_ref, mean_ref, variance_ref, normed):
    here = lax.axis_index("c") == lax.axis_index("zl")
    rows = jnp.where(here, mine[...], other[...]).astype(jnp.float32)
    streams = 1 + TANGENTS
    gain = gain_ref[...]
    normed[...] = jnp.zeros_like(normed)
    for image in range(mean_ref.shape[0]):
        at = image * streams
        x = rows[at : at + 1]
        c = x - row_mean(x)
        r = lax.rsqrt(row_mean(c * c) + epsilon)
        normed[at : at + 1] = c * r * gain
        for j in range(1, streams):
            t = rows[at + j : at + j + 1]
            dc = t - row_mean(t)
            dr = -(r * r * r) * row_mean(c * dc)
            normed[at + j : at + j + 1] = (dc * r + c * dr) * gain
    logits = dot(normed[...].astype(jnp.bfloat16), head_ref[...])
    for image in range(mean_ref.shape[0]):
        at = image * streams
        mean_ref[image] = logits[at : at + 1]
        tangents = [logits[at + j : at + j + 1] for j in range(1, streams)]
        variance_ref[image] = sum(t * t for t in tangents)


def final_logits(mine, other, gain, head, micro):
    shape = jax.ShapeDtypeStruct((micro, 1, head.shape[1]), jnp.float32)
    return pl.pallas_call(
        final_body,
        out_shape=(shape, shape),
        in_specs=[VMEM_SPEC] * 4,
        out_specs=(VMEM_SPEC,) * 2,
        scratch_shapes=[vmem(mine.shape, jnp.float32)],
        compiler_params=limit(),
        name="final_logits",
    )(mine, other, gain, head)


def shards(tokens, w_qkv, w_output, tangent_value, tangent_output, layer_gain, final_gain, head):
    micro, _, length, width = tokens.shape
    images = tokens.reshape(micro, length, width)
    packed = pack(w_qkv, tangent_value, w_output, tangent_output)
    weights, (images, gain, order) = gathered(packed, layer_gain, images)

    stages = 8
    streams = (None,) * (1 + TANGENTS)
    last = []
    for step in range(stages + micro - 1):
        route = [(s, s + 1) for s in range(stages - 1) if 0 <= step - s < micro]
        out, normed, qkv, probs, attended = primal_layer(step, images, streams[0], gain, weights)
        results, moved = [out], []
        if route:
            moved.append(lax.ppermute(out, ("zh", "zl"), route))
        saved = (qkv, probs, *shared_layer(step, weights, normed, attended))
        for which in range(TANGENTS):
            out = tangent_layer(
                which, step, images, streams[0], streams[1 + which], gain, weights, saved
            )
            results.append(out)
            if route:
                moved.append(lax.ppermute(out, ("zh", "zl"), route))
        streams = tuple(moved)
        if step >= stages - 1:
            last += results
    rows = class_rows(order, last)
    sent = [
        lax.ppermute(rows, ("zh", "c", "zl"), [(13, 4 * i), (15, 4 * i + 3)]) for i in range(4)
    ]
    mine = one_of(sent)
    return final_logits(mine, core_swap(mine), final_gain[None], head, micro)


def solution(mesh):
    sizes = (4, 2, 8, 4, 2)
    split = Mesh(mesh.devices.reshape(sizes), ("zh", "c", "y", "x", "zl"))
    section, dp = ("zh", "c"), ("y", "x", "zl")
    return jax.shard_map(
        shards,
        mesh=split,
        in_specs=(
            P(None, dp, None, None),
            P(section, dp, None),
            P(section, None, dp),
            P(section, None, dp, None),
            P(section, None, None, dp),
            P(section, None),
            P(),
            P(None, section),
        ),
        out_specs=(P(None, dp, section), P(None, dp, section)),
        check_vma=False,
    )
```

```python
import functools

import jax
import jax.numpy as jnp
from jax import lax
from jax.experimental import pallas as pl
from jax.experimental.pallas import tpu as pltpu
from jax.sharding import Mesh
from jax.sharding import PartitionSpec as P

HEADS = 8
HEAD = 64
TANGENTS = 2
HD = 512
PAIR = 2 * HEAD
PAIRS = HEADS // 2
SCALE = HEAD ** (-0.5)

epsilon = 1e-06
GAIN_PARTS = 3
GAIN_ROWS = 8

QKV = slice(0, 3 * HD)
TV = (slice(3 * HD, 4 * HD), slice(4 * HD, 5 * HD))
WO = slice(5 * HD, 6 * HD)
TO = (slice(6 * HD, 7 * HD), slice(7 * HD, 8 * HD))


VMEM_SPEC = pl.BlockSpec(memory_space=pltpu.VMEM)
HBM_SPEC = pl.BlockSpec(memory_space=pltpu.HBM)


def dot(left, right):
    return jnp.dot(left, right, preferred_element_type=jnp.float32)


def dot_t(left, right):
    return lax.dot_general(
        left, right, (((1,), (1,)), ((), ())), preferred_element_type=jnp.float32
    )


def row_mean(a):
    return jnp.sum(a, -1, keepdims=True) * (1.0 / a.shape[-1])


def head_masks(rows):
    lane = lax.broadcasted_iota(jnp.int32, (rows, PAIR), 1)
    return lane < HEAD, lane >= HEAD


def part(ref, which, pair):
    at = which * HD + pair * PAIR
    return ref[:, at : at + PAIR]


def masked(a, mask):
    return jnp.where(mask, a, jnp.zeros_like(a))


def plane_of_this():
    return 2 * lax.axis_index("zh") + lax.axis_index("zl")


def working(step, plane):
    return (step - plane >= 0) & (step - plane < 2)


def entering(step, plane, images, stream, t_stream=None):
    if step < 2:
        x = images[step].astype(jnp.float32)
        t = jnp.zeros_like(x)
        if step == 1:
            x = jnp.where(plane == 0, x, stream[...].astype(jnp.float32))
            if t_stream is not None:
                t = jnp.where(plane == 0, t, t_stream[...].astype(jnp.float32))
        return x, t
    return (
        stream[...].astype(jnp.float32),
        None if t_stream is None else t_stream[...].astype(jnp.float32),
    )


def primal_body(step, *refs):
    gain_ref, w_ref, out_ref, n_ref, qkv_ref, p_ref, att_ref = refs[-7:]
    images, streams = refs[0] if step < 2 else None, refs[1 if step < 2 else 0 : -7]
    plane = plane_of_this()

    @pl.when(working(step, plane))
    def _():
        x, _ = entering(step, plane, images, *streams[:1] or (None,))
        gain = gain_ref[...]
        c = x - row_mean(x)
        r = lax.rsqrt(row_mean(c * c) + epsilon)
        n = (c * r * gain).astype(jnp.bfloat16)
        n_ref[...] = n
        qkv_ref[...] = dot(n, w_ref[:, QKV]).astype(jnp.bfloat16)
        masks = head_masks(x.shape[0])
        for pair in range(PAIRS):
            q, k, v = (part(qkv_ref, i, pair) for i in range(3))
            total = None
            for half in range(2):
                s = dot_t(masked(q, masks[half]), k) * SCALE
                e = jnp.exp(s - jnp.max(s, -1, keepdims=True))
                p = e / jnp.sum(e, -1, keepdims=True)
                p_ref[2 * pair + half] = p
                a = dot(p.astype(jnp.bfloat16), masked(v, masks[half]))
                total = a if total is None else total + a
            att_ref[:, pair * PAIR : (pair + 1) * PAIR] = total.astype(jnp.bfloat16)
        out_ref[...] = (x + dot_t(att_ref[...], w_ref[:, WO])).astype(jnp.bfloat16)


def shared_body(step, w_ref, n_ref, att_ref, values_ref, outs_ref):
    @pl.when(working(step, plane_of_this()))
    def _():
        for which in range(TANGENTS):
            values_ref[which] = dot(n_ref[...], w_ref[:, TV[which]])
            outs_ref[which] = dot_t(att_ref[...], w_ref[:, TO[which]])


def tangent_body(which, step, *refs):
    gain_ref, w_ref, qkv_ref, p_ref, values_ref, outs_ref, out_ref, mine, joined = refs[-9:]
    images, streams = refs[0] if step < 2 else None, refs[1 if step < 2 else 0 : -9]
    plane = plane_of_this()

    @pl.when(working(step, plane))
    def _():
        x, t = entering(step, plane, images, *(streams or (None, None)))
        gain = gain_ref[...]
        c = x - row_mean(x)
        r = lax.rsqrt(row_mean(c * c) + epsilon)
        dc = t - row_mean(t)
        dr = -(r * r * r) * row_mean(c * dc)
        dn = ((dc * r + c * dr) * gain).astype(jnp.bfloat16)
        mine[:, : 2 * HD] = dot(dn, w_ref[:, : 2 * HD]).astype(jnp.bfloat16)
        values = dot(dn, w_ref[:, 2 * HD : 3 * HD]) + values_ref[which]
        mine[:, 2 * HD :] = values.astype(jnp.bfloat16)
        masks = head_masks(x.shape[0])
        for pair in range(PAIRS):
            q0, k0, v0 = (part(qkv_ref, i, pair) for i in range(3))
            q1, k1, v1 = (part(mine, i, pair) for i in range(3))
            total = None
            for half in range(2):
                m = masks[half]
                ds = (dot_t(masked(q1, m), k0) + dot_t(masked(q0, m), k1)) * SCALE
                p = p_ref[2 * pair + half]
                dp = p * (ds - jnp.sum(p * ds, -1, keepdims=True))
                a = dot(dp.astype(jnp.bfloat16), masked(v0, m)) + dot(
                    p.astype(jnp.bfloat16), masked(v1, m)
                )
                total = a if total is None else total + a
            joined[:, pair * PAIR : (pair + 1) * PAIR] = total.astype(jnp.bfloat16)
        moved = dot_t(joined[...], w_ref[:, WO]) + outs_ref[which]
        out_ref[...] = (t + moved).astype(jnp.bfloat16)


def cost(flops, bytes_accessed):
    return pl.CostEstimate(flops=flops, bytes_accessed=bytes_accessed, transcendentals=0)


def vmem(shape, dtype=jnp.bfloat16):
    return pltpu.VMEM(shape, dtype)


def in_hbm(a):
    return pltpu.with_memory_space_constraint(a, pltpu.HBM)


def limit(mib=4):
    return pltpu.CompilerParams(vmem_limit_bytes=mib << 20)


def primal_layer(step, images, x, gain, weights):
    tokens, width = images.shape[1:]
    bf16 = jnp.bfloat16
    given = (*((images,) if step < 2 else ()), *((x,) if step else ()), gain, weights)
    return pl.pallas_call(
        functools.partial(primal_body, step),
        out_shape=(
            jax.ShapeDtypeStruct((tokens, width), bf16),
            jax.ShapeDtypeStruct((tokens, width), bf16),
            jax.ShapeDtypeStruct((tokens, 3 * HD), bf16),
            jax.ShapeDtypeStruct((HEADS, tokens, tokens), jnp.float32),
            jax.ShapeDtypeStruct((tokens, HD), bf16),
        ),
        in_specs=[VMEM_SPEC] * len(given),
        out_specs=(VMEM_SPEC,) * 5,
        cost_estimate=cost(2 * tokens * width * 4 * HD, 1 << 20),
        compiler_params=limit(12),
        name="primal_layer",
    )(*given)


def shared_layer(step, weights, normed, attended):
    tokens, width = normed.shape
    return pl.pallas_call(
        functools.partial(shared_body, step),
        out_shape=(
            jax.ShapeDtypeStruct((TANGENTS, tokens, HD), jnp.float32),
            jax.ShapeDtypeStruct((TANGENTS, tokens, width), jnp.float32),
        ),
        in_specs=[VMEM_SPEC] * 3,
        out_specs=(VMEM_SPEC,) * 2,
        cost_estimate=cost(2 * tokens * width * 4 * HD, 1 << 20),
        compiler_params=limit(12),
        name="shared_layer",
    )(weights, normed, attended)


def tangent_layer(which, step, images, x, t, gain, weights, saved):
    tokens, width = images.shape[1:]
    given = (*((images,) if step < 2 else ()), *((x, t) if step else ()), gain, weights, *saved)
    return pl.pallas_call(
        functools.partial(tangent_body, which, step),
        out_shape=jax.ShapeDtypeStruct((tokens, width), jnp.bfloat16),
        in_specs=[VMEM_SPEC] * len(given),
        out_specs=VMEM_SPEC,
        scratch_shapes=[vmem((tokens, 3 * HD)), vmem((tokens, HD))],
        cost_estimate=cost(2 * tokens * width * 4 * HD, 1 << 20),
        compiler_params=limit(12),
    )(*given)


def copied(pairs, sems):
    copies = [pltpu.make_async_copy(a, b, sems.at[i]) for i, (a, b) in enumerate(pairs)]
    for copy in copies:
        copy.start()
    for copy in copies:
        copy.wait()


def pack_body(qkv, value, output, tangent_output, gain, out, out_gain, held, sems):
    pairs = [(qkv.at[0], out.at[:, QKV]), (output.at[0], out.at[:, WO]), (gain, held)]
    for which in range(TANGENTS):
        pairs.append((value.at[0, which], out.at[:, TV[which]]))
        pairs.append((tangent_output.at[0, which], out.at[:, TO[which]]))
    copied(pairs, sems)
    rows = out.shape[0]
    out_gain[:rows] = out[...]
    rest, width = held[...], held.shape[1]
    for i in range(GAIN_PARTS):
        high = rest.astype(jnp.bfloat16).astype(jnp.float32)
        rest = rest - high
        spread = jnp.broadcast_to(high, (GAIN_ROWS, width)).astype(jnp.bfloat16)
        out_gain[rows:, i * width : (i + 1) * width] = spread
    out_gain[rows:, GAIN_PARTS * width :] = jnp.zeros((GAIN_ROWS, width), jnp.bfloat16)


def pack(w_qkv, tangent_value, w_output, tangent_output, gain):
    shares = (w_qkv, tangent_value, w_output.swapaxes(1, 2), tangent_output.swapaxes(2, 3), gain)
    rows = w_qkv.shape[1]
    return pl.pallas_call(
        pack_body,
        out_shape=(vmem((rows, 8 * HD)), vmem((rows + GAIN_ROWS, 8 * HD))),
        in_specs=[HBM_SPEC] * 5,
        out_specs=(VMEM_SPEC,) * 2,
        scratch_shapes=[vmem(gain.shape, jnp.float32), pltpu.SemaphoreType.DMA((3 + 2 * TANGENTS,))],
        compiler_params=limit(),
        name="pack",
    )(*map(in_hbm, shares))


def line_body(rows, *refs):
    parts, out = refs[:-1], refs[-1]
    at = 0
    for part in parts:
        count = min(rows, part.shape[0])
        out[at : at + count] = part[:count]
        at += count


def line_up(parts, rows=1024):
    count, columns = sum(min(rows, p.shape[0]) for p in parts), parts[0].shape[1]
    return pl.pallas_call(
        functools.partial(line_body, rows),
        out_shape=vmem((count, columns)),
        in_specs=[VMEM_SPEC] * len(parts),
        out_specs=VMEM_SPEC,
        compiler_params=limit(),
        name="line_up",
    )(*parts)


def half_body(first, whole, out):
    out[...] = whole[first : first + out.shape[0]]


def half_of(whole, upper):
    rows, columns = whole.shape
    return pl.pallas_call(
        functools.partial(half_body, upper * (rows // 2)),
        out_shape=vmem((rows // 2, columns)),
        in_specs=[VMEM_SPEC],
        out_specs=VMEM_SPEC,
        compiler_params=limit(),
        name="half_of",
    )(whole)


def order_body(tokens, own_tokens, given, images_out, gain_out, order_out):
    core, y, x = lax.axis_index("c"), lax.axis_index("y"), lax.axis_index("x")
    width = order_out.shape[0]
    place = lax.broadcasted_iota(jnp.int32, (1, width), 1)
    half, row = place // (width // 2), place % (width // 2)
    piece, share, element = row // 64, row % 64 // 16, row % 16
    rise = jnp.where(piece % 2 == 1, -((piece + 1) // 2), piece // 2)
    along = jnp.where(share <= 1, -share, share - 1)
    at = ((y + rise + 8) % 8 * 4 + (x + along + 4) % 4) * 2 + (core + half) % 2
    feature = at * 16 + element
    one_hot = lax.broadcasted_iota(jnp.int32, (width, width), 0) == feature
    order_out[...] = one_hot.astype(jnp.float32).astype(jnp.bfloat16)
    order = order_out[...]
    for i in range(images_out.shape[0]):
        mine = jnp.where(core == 0, own_tokens[i], tokens[i])
        images_out[i] = dot(mine, order).astype(jnp.bfloat16)
    below = given.shape[0] - GAIN_ROWS
    gain = jnp.zeros((GAIN_ROWS, width), jnp.float32)
    for i in range(GAIN_PARTS):
        gain = gain + dot(given[below:, i * width : (i + 1) * width], order)
    gain_out[...] = gain[:1]


def in_order(tokens, own_tokens, share):
    width = tokens.shape[-1]
    return pl.pallas_call(
        order_body,
        out_shape=(vmem(tokens.shape), vmem((1, width), jnp.float32), vmem((width, width))),
        in_specs=[VMEM_SPEC] * 3,
        out_specs=(VMEM_SPEC,) * 3,
        compiler_params=limit(12),
        cost_estimate=cost(1 << 26, 1 << 20),
        name="in_order",
    )(tokens, own_tokens, share)


def assemble_body(first, aliased, *refs):
    pieces, out = refs[int(aliased) : -1], refs[-1]
    for at, piece in zip(first, pieces, strict=True):
        out[at : at + piece.shape[0]] = piece[...]


def assemble(base, first, pieces):
    columns = pieces[0].shape[1]
    given = [] if base is None else [base]
    return pl.pallas_call(
        functools.partial(assemble_body, first, base is not None),
        out_shape=vmem((1024, columns)),
        in_specs=[VMEM_SPEC] * (len(given) + len(pieces)),
        out_specs=VMEM_SPEC,
        input_output_aliases={0: 0} if given else {},
        cost_estimate=cost(1 << 24, 1 << 20),
        compiler_params=limit(),
        name="assemble",
    )(*given, *pieces)


def core_swap(a):
    return lax.ppermute(a, "c", [(0, 1), (1, 0)])


def gathered(packed, packed_gain, images):
    def moves(d):
        cells = [(c, x, z) for c in range(2) for x in range(4) for z in range(2)]
        return [(8 * c + 2 * x + z, 8 * z + 2 * ((x + d) % 4) + c) for c, x, z in cells]

    def up_ring(a):
        return lax.ppermute(a, "y", [(j, (j + 1) % 8) for j in range(8)])

    def down_ring(a):
        return lax.ppermute(a, "y", [(j, (j - 1) % 8) for j in range(8)])

    def to_pair(a):
        return lax.ppermute(a, ("c", "zl"), [(3, 2)])

    shares = [
        lax.ppermute(packed if d else packed_gain, ("c", "x", "zl"), moves(d)) for d in (0, 1, -1, 2)
    ]
    line = line_up(shares, packed.shape[0])
    up_1 = up_ring(line)
    down_1 = down_ring(line)
    beside = to_pair(images)
    ordered = in_order(beside, images, shares[0])
    up_1, ordered = lax.optimization_barrier((up_1, ordered))
    up_2 = up_ring(up_1)
    early = line_up([line, up_1])
    down_1, early = lax.optimization_barrier((down_1, early))
    down_2 = down_ring(down_1)
    first = line_up([early, down_1])
    other_first = core_swap(first)
    up_2, other_first = lax.optimization_barrier((up_2, other_first))
    up_3 = up_ring(up_2)
    early = line_up([up_2])
    down_2, early = lax.optimization_barrier((down_2, early))
    down_3 = down_ring(down_2)
    second = line_up([early, down_2])
    other_second = core_swap(second)
    up_3, other_second = lax.optimization_barrier((up_3, other_second))
    up_4 = up_ring(half_of(up_3, 0))
    down_4 = down_ring(half_of(down_3, 1))
    third = line_up([up_3, down_3])
    other_third = core_swap(third)
    up_4, other_third = lax.optimization_barrier((up_4, other_third))
    fourth = line_up([up_4, down_4])
    other_fourth = core_swap(fourth)
    pieces = (first, second, third, fourth, other_first, other_second, other_third)
    base = assemble(None, (0, 192, 320, 448, 512, 704, 832), pieces)
    return assemble(base, (960,), (other_fourth,)), ordered


def rows_body(*refs):
    order, streams, out, rows = refs[0], refs[1:-2], refs[-2], refs[-1]
    rows[...] = jnp.zeros_like(rows)
    for i, stream in enumerate(streams):
        rows[i : i + 1] = stream[0:1].astype(jnp.float32)
    out[...] = dot_t(rows[...].astype(jnp.bfloat16), order[...]).astype(jnp.bfloat16)


def class_rows(order, streams):
    width = streams[0].shape[1]
    return pl.pallas_call(
        rows_body,
        out_shape=vmem((8, width)),
        in_specs=[VMEM_SPEC] * (1 + len(streams)),
        out_specs=VMEM_SPEC,
        scratch_shapes=[vmem((8, width), jnp.float32)],
        compiler_params=limit(),
        name="class_rows",
    )(order, *streams)


def sum_body(*refs):
    total = refs[0][...]
    for ref in refs[1:-1]:
        total = total + ref[...]
    refs[-1][...] = total


def one_of(parts):
    return pl.pallas_call(
        sum_body,
        out_shape=vmem(parts[0].shape),
        in_specs=[VMEM_SPEC] * len(parts),
        out_specs=VMEM_SPEC,
        compiler_params=limit(),
        name="one_of",
    )(*parts)


def final_body(mine, other, gain_ref, head_ref, mean_ref, variance_ref, normed):
    here = lax.axis_index("c") == lax.axis_index("zl")
    rows = jnp.where(here, mine[...], other[...]).astype(jnp.float32)
    streams = 1 + TANGENTS
    gain = gain_ref[...]
    normed[...] = jnp.zeros_like(normed)
    for image in range(mean_ref.shape[0]):
        at = image * streams
        x = rows[at : at + 1]
        c = x - row_mean(x)
        r = lax.rsqrt(row_mean(c * c) + epsilon)
        normed[at : at + 1] = c * r * gain
        for j in range(1, streams):
            t = rows[at + j : at + j + 1]
            dc = t - row_mean(t)
            dr = -(r * r * r) * row_mean(c * dc)
            normed[at + j : at + j + 1] = (dc * r + c * dr) * gain
    logits = dot(normed[...].astype(jnp.bfloat16), head_ref[...])
    for image in range(mean_ref.shape[0]):
        at = image * streams
        mean_ref[image] = logits[at : at + 1]
        tangents = [logits[at + j : at + j + 1] for j in range(1, streams)]
        variance_ref[image] = sum(t * t for t in tangents)


def final_logits(mine, other, gain, head, micro):
    shape = jax.ShapeDtypeStruct((micro, 1, head.shape[1]), jnp.float32)
    return pl.pallas_call(
        final_body,
        out_shape=(shape, shape),
        in_specs=[VMEM_SPEC] * 4,
        out_specs=(VMEM_SPEC,) * 2,
        scratch_shapes=[vmem(mine.shape, jnp.float32)],
        compiler_params=limit(),
        name="final_logits",
    )(mine, other, gain, head)


def shards(tokens, w_qkv, w_output, tangent_value, tangent_output, layer_gain, final_gain, head):
    micro, _, length, width = tokens.shape
    images = tokens.reshape(micro, length, width)
    packed, packed_gain = pack(w_qkv, tangent_value, w_output, tangent_output, layer_gain)
    weights, (images, gain, order) = gathered(packed, packed_gain, images)

    stages = 8
    streams = (None,) * (1 + TANGENTS)
    last = []
    for step in range(stages + micro - 1):
        route = [(s, s + 1) for s in range(stages - 1) if 0 <= step - s < micro]
        out, normed, qkv, probs, attended = primal_layer(step, images, streams[0], gain, weights)
        results, moved = [out], []
        if route:
            moved.append(lax.ppermute(out, ("zh", "zl"), route))
        saved = (qkv, probs, *shared_layer(step, weights, normed, attended))
        for which in range(TANGENTS):
            out = tangent_layer(
                which, step, images, streams[0], streams[1 + which], gain, weights, saved
            )
            results.append(out)
            if route:
                moved.append(lax.ppermute(out, ("zh", "zl"), route))
        streams = tuple(moved)
        if step >= stages - 1:
            last += results
    rows = class_rows(order, last)
    sent = [
        lax.ppermute(rows, ("zh", "c", "zl"), [(13, 4 * i), (15, 4 * i + 3)]) for i in range(4)
    ]
    mine = one_of(sent)
    return final_logits(mine, core_swap(mine), final_gain[None], head, micro)


def solution(mesh):
    sizes = (4, 2, 8, 4, 2)
    split = Mesh(mesh.devices.reshape(sizes), ("zh", "c", "y", "x", "zl"))
    section, dp = ("zh", "c"), ("y", "x", "zl")
    return jax.shard_map(
        shards,
        mesh=split,
        in_specs=(
            P(None, dp, None, None),
            P(section, dp, None),
            P(section, None, dp),
            P(section, None, dp, None),
            P(section, None, None, dp),
            P(section, None),
            P(),
            P(None, section),
        ),
        out_specs=(P(None, dp, section), P(None, dp, section)),
        check_vma=False,
    )
```

```python
import functools

import jax
import jax.numpy as jnp
from jax import lax
from jax.experimental import pallas as pl
from jax.experimental.pallas import tpu as pltpu
from jax.sharding import Mesh
from jax.sharding import PartitionSpec as P

HEADS = 8
HEAD = 64
TANGENTS = 2
HD = 512
PAIR = 2 * HEAD
PAIRS = HEADS // 2
SCALE = HEAD ** (-0.5)

epsilon = 1e-06

QKV = slice(0, 3 * HD)
TV = (slice(3 * HD, 4 * HD), slice(4 * HD, 5 * HD))
WO = slice(5 * HD, 6 * HD)
TO = (slice(6 * HD, 7 * HD), slice(7 * HD, 8 * HD))


VMEM_SPEC = pl.BlockSpec(memory_space=pltpu.VMEM)
HBM_SPEC = pl.BlockSpec(memory_space=pltpu.HBM)


def dot(left, right):
    return jnp.dot(left, right, preferred_element_type=jnp.float32)


def dot_t(left, right):
    return lax.dot_general(
        left, right, (((1,), (1,)), ((), ())), preferred_element_type=jnp.float32
    )


def row_mean(a):
    return jnp.sum(a, -1, keepdims=True) * (1.0 / a.shape[-1])


def head_masks(rows):
    lane = lax.broadcasted_iota(jnp.int32, (rows, PAIR), 1)
    return lane < HEAD, lane >= HEAD


def part(ref, which, pair):
    at = which * HD + pair * PAIR
    return ref[:, at : at + PAIR]


def masked(a, mask):
    return jnp.where(mask, a, jnp.zeros_like(a))


def plane_of_this():
    return 2 * lax.axis_index("zh") + lax.axis_index("zl")


def working(step, plane):
    return (step - plane >= 0) & (step - plane < 2)


def entering(step, plane, images, stream, t_stream=None):
    if step < 2:
        x = images[step].astype(jnp.float32)
        t = jnp.zeros_like(x)
        if step == 1:
            x = jnp.where(plane == 0, x, stream[...].astype(jnp.float32))
            if t_stream is not None:
                t = jnp.where(plane == 0, t, t_stream[...].astype(jnp.float32))
        return x, t
    return (
        stream[...].astype(jnp.float32),
        None if t_stream is None else t_stream[...].astype(jnp.float32),
    )


def primal_body(step, *refs):
    gain_ref, w_ref, out_ref, n_ref, qkv_ref, p_ref, att_ref = refs[-7:]
    images, streams = refs[0] if step < 2 else None, refs[1 if step < 2 else 0 : -7]
    plane = plane_of_this()

    @pl.when(working(step, plane))
    def _():
        x, _ = entering(step, plane, images, *streams[:1] or (None,))
        gain = gain_ref[...]
        c = x - row_mean(x)
        r = lax.rsqrt(row_mean(c * c) + epsilon)
        n = (c * r * gain).astype(jnp.bfloat16)
        n_ref[...] = n
        qkv_ref[...] = dot(n, w_ref[:, QKV]).astype(jnp.bfloat16)
        masks = head_masks(x.shape[0])
        for pair in range(PAIRS):
            q, k, v = (part(qkv_ref, i, pair) for i in range(3))
            total = None
            for half in range(2):
                s = dot_t(masked(q, masks[half]), k) * SCALE
                e = jnp.exp(s - jnp.max(s, -1, keepdims=True))
                p = e / jnp.sum(e, -1, keepdims=True)
                p_ref[2 * pair + half] = p
                a = dot(p.astype(jnp.bfloat16), masked(v, masks[half]))
                total = a if total is None else total + a
            att_ref[:, pair * PAIR : (pair + 1) * PAIR] = total.astype(jnp.bfloat16)
        out_ref[...] = (x + dot_t(att_ref[...], w_ref[:, WO])).astype(jnp.bfloat16)


def shared_body(step, w_ref, n_ref, att_ref, values_ref, outs_ref):
    @pl.when(working(step, plane_of_this()))
    def _():
        for which in range(TANGENTS):
            values_ref[which] = dot(n_ref[...], w_ref[:, TV[which]])
            outs_ref[which] = dot_t(att_ref[...], w_ref[:, TO[which]])


def tangent_body(which, step, *refs):
    gain_ref, w_ref, qkv_ref, p_ref, values_ref, outs_ref, out_ref, mine, joined = refs[-9:]
    images, streams = refs[0] if step < 2 else None, refs[1 if step < 2 else 0 : -9]
    plane = plane_of_this()

    @pl.when(working(step, plane))
    def _():
        x, t = entering(step, plane, images, *(streams or (None, None)))
        gain = gain_ref[...]
        c = x - row_mean(x)
        r = lax.rsqrt(row_mean(c * c) + epsilon)
        dc = t - row_mean(t)
        dr = -(r * r * r) * row_mean(c * dc)
        dn = ((dc * r + c * dr) * gain).astype(jnp.bfloat16)
        mine[:, : 2 * HD] = dot(dn, w_ref[:, : 2 * HD]).astype(jnp.bfloat16)
        values = dot(dn, w_ref[:, 2 * HD : 3 * HD]) + values_ref[which]
        mine[:, 2 * HD :] = values.astype(jnp.bfloat16)
        masks = head_masks(x.shape[0])
        for pair in range(PAIRS):
            q0, k0, v0 = (part(qkv_ref, i, pair) for i in range(3))
            q1, k1, v1 = (part(mine, i, pair) for i in range(3))
            total = None
            for half in range(2):
                m = masks[half]
                ds = (dot_t(masked(q1, m), k0) + dot_t(masked(q0, m), k1)) * SCALE
                p = p_ref[2 * pair + half]
                dp = p * (ds - jnp.sum(p * ds, -1, keepdims=True))
                a = dot(dp.astype(jnp.bfloat16), masked(v0, m)) + dot(
                    p.astype(jnp.bfloat16), masked(v1, m)
                )
                total = a if total is None else total + a
            joined[:, pair * PAIR : (pair + 1) * PAIR] = total.astype(jnp.bfloat16)
        moved = dot_t(joined[...], w_ref[:, WO]) + outs_ref[which]
        out_ref[...] = (t + moved).astype(jnp.bfloat16)


def cost(flops, bytes_accessed):
    return pl.CostEstimate(flops=flops, bytes_accessed=bytes_accessed, transcendentals=0)


def vmem(shape, dtype=jnp.bfloat16):
    return pltpu.VMEM(shape, dtype)


def in_hbm(a):
    return pltpu.with_memory_space_constraint(a, pltpu.HBM)


def limit(mib=4):
    return pltpu.CompilerParams(vmem_limit_bytes=mib << 20)


def primal_layer(step, images, x, gain, weights):
    tokens, width = images.shape[1:]
    bf16 = jnp.bfloat16
    given = (*((images,) if step < 2 else ()), *((x,) if step else ()), gain, weights)
    return pl.pallas_call(
        functools.partial(primal_body, step),
        out_shape=(
            jax.ShapeDtypeStruct((tokens, width), bf16),
            jax.ShapeDtypeStruct((tokens, width), bf16),
            jax.ShapeDtypeStruct((tokens, 3 * HD), bf16),
            jax.ShapeDtypeStruct((HEADS, tokens, tokens), jnp.float32),
            jax.ShapeDtypeStruct((tokens, HD), bf16),
        ),
        in_specs=[VMEM_SPEC] * len(given),
        out_specs=(VMEM_SPEC,) * 5,
        cost_estimate=cost(2 * tokens * width * 4 * HD, 1 << 20),
        compiler_params=limit(12),
        name="primal_layer",
    )(*given)


def shared_layer(step, weights, normed, attended):
    tokens, width = normed.shape
    return pl.pallas_call(
        functools.partial(shared_body, step),
        out_shape=(
            jax.ShapeDtypeStruct((TANGENTS, tokens, HD), jnp.float32),
            jax.ShapeDtypeStruct((TANGENTS, tokens, width), jnp.float32),
        ),
        in_specs=[VMEM_SPEC] * 3,
        out_specs=(VMEM_SPEC,) * 2,
        cost_estimate=cost(2 * tokens * width * 4 * HD, 1 << 20),
        compiler_params=limit(12),
        name="shared_layer",
    )(weights, normed, attended)


def tangent_layer(which, step, images, x, t, gain, weights, saved):
    tokens, width = images.shape[1:]
    given = (*((images,) if step < 2 else ()), *((x, t) if step else ()), gain, weights, *saved)
    return pl.pallas_call(
        functools.partial(tangent_body, which, step),
        out_shape=jax.ShapeDtypeStruct((tokens, width), jnp.bfloat16),
        in_specs=[VMEM_SPEC] * len(given),
        out_specs=VMEM_SPEC,
        scratch_shapes=[vmem((tokens, 3 * HD)), vmem((tokens, HD))],
        cost_estimate=cost(2 * tokens * width * 4 * HD, 1 << 20),
        compiler_params=limit(12),
    )(*given)


def copied(pairs, sems):
    copies = [pltpu.make_async_copy(a, b, sems.at[i]) for i, (a, b) in enumerate(pairs)]
    for copy in copies:
        copy.start()
    for copy in copies:
        copy.wait()


def pack_body(qkv, value, output, tangent_output, out, sems):
    pairs = [(qkv.at[0], out.at[:, QKV]), (output.at[0], out.at[:, WO])]
    for which in range(TANGENTS):
        pairs.append((value.at[0, which], out.at[:, TV[which]]))
        pairs.append((tangent_output.at[0, which], out.at[:, TO[which]]))
    copied(pairs, sems)


def pack(w_qkv, tangent_value, w_output, tangent_output):
    shares = (w_qkv, tangent_value, w_output.swapaxes(1, 2), tangent_output.swapaxes(2, 3))
    return pl.pallas_call(
        pack_body,
        out_shape=vmem((w_qkv.shape[1], 8 * HD)),
        in_specs=[HBM_SPEC] * 4,
        out_specs=VMEM_SPEC,
        scratch_shapes=[pltpu.SemaphoreType.DMA((2 + 2 * TANGENTS,))],
        compiler_params=limit(),
        name="pack",
    )(*map(in_hbm, shares))


def line_body(*refs):
    parts, out = refs[:-1], refs[-1]
    at = 0
    for part in parts:
        out[at : at + part.shape[0]] = part[...]
        at += part.shape[0]


def line_up(parts):
    rows, columns = sum(p.shape[0] for p in parts), parts[0].shape[1]
    return pl.pallas_call(
        line_body,
        out_shape=vmem((rows, columns)),
        in_specs=[VMEM_SPEC] * len(parts),
        out_specs=VMEM_SPEC,
        compiler_params=limit(),
        name="line_up",
    )(*parts)


def half_body(first, whole, out):
    out[...] = whole[first : first + out.shape[0]]


def half_of(whole, upper):
    rows, columns = whole.shape
    return pl.pallas_call(
        functools.partial(half_body, upper * (rows // 2)),
        out_shape=vmem((rows // 2, columns)),
        in_specs=[VMEM_SPEC],
        out_specs=VMEM_SPEC,
        compiler_params=limit(),
        name="half_of",
    )(whole)


def order_body(tokens, own_tokens, own_gain, other_gain, images_out, gain_out, order_out):
    core, y, x = lax.axis_index("c"), lax.axis_index("y"), lax.axis_index("x")
    width = order_out.shape[0]
    place = lax.broadcasted_iota(jnp.int32, (1, width), 1)
    half, row = place // (width // 2), place % (width // 2)
    piece, share, element = row // 64, row % 64 // 16, row % 16
    rise = jnp.where(piece % 2 == 1, -((piece + 1) // 2), piece // 2)
    along = jnp.where(share <= 1, -share, share - 1)
    at = ((y + rise + 8) % 8 * 4 + (x + along + 4) % 4) * 2 + half
    feature = at * 16 + element
    one_hot = lax.broadcasted_iota(jnp.int32, (width, width), 0) == feature
    order_out[...] = one_hot.astype(jnp.float32).astype(jnp.bfloat16)
    order = order_out[...]
    for i in range(images_out.shape[0]):
        mine = jnp.where(core == 0, own_tokens[i], tokens[i])
        images_out[i] = dot(mine, order).astype(jnp.bfloat16)
    rest = jnp.where(core == lax.axis_index("zl"), own_gain[...], other_gain[...])
    gain = jnp.zeros_like(rest)
    for _ in range(3):
        high = rest.astype(jnp.bfloat16)
        rest = rest - high.astype(jnp.float32)
        gain = gain + dot(jnp.broadcast_to(high, (8, width)), order)[:1]
    gain_out[...] = gain


def in_order(tokens, own_tokens, own_gain, other_gain):
    width = tokens.shape[-1]
    return pl.pallas_call(
        order_body,
        out_shape=(vmem(tokens.shape), vmem(own_gain.shape, jnp.float32), vmem((width, width))),
        in_specs=[VMEM_SPEC] * 4,
        out_specs=(VMEM_SPEC,) * 3,
        compiler_params=limit(12),
        cost_estimate=cost(1 << 26, 1 << 20),
        name="in_order",
    )(tokens, own_tokens, own_gain, other_gain)


def assemble_body(first, aliased, *refs):
    pieces, out = refs[int(aliased) : -1], refs[-1]
    core, half = lax.axis_index("c"), out.shape[0] // 2
    for (at, other), piece in zip(first, pieces, strict=True):
        rows = piece.shape[0]
        at = at + half * (1 - core if other else core)
        out[pl.ds(pl.multiple_of(at, 64), rows)] = piece[...]


def assemble(base, first, pieces):
    columns = pieces[0].shape[1]
    given = [] if base is None else [base]
    return pl.pallas_call(
        functools.partial(assemble_body, first, base is not None),
        out_shape=vmem((1024, columns)),
        in_specs=[VMEM_SPEC] * (len(given) + len(pieces)),
        out_specs=VMEM_SPEC,
        input_output_aliases={0: 0} if given else {},
        cost_estimate=cost(1 << 24, 1 << 20),
        compiler_params=limit(),
        name="assemble",
    )(*given, *pieces)


def core_swap(a):
    return lax.ppermute(a, "c", [(0, 1), (1, 0)])


def gathered(packed, gain, images):
    def moves(d):
        cells = [(c, x, z) for c in range(2) for x in range(4) for z in range(2)]
        return [(8 * c + 2 * x + z, 8 * z + 2 * ((x + d) % 4) + c) for c, x, z in cells]

    def up_ring(a):
        return lax.ppermute(a, "y", [(j, (j + 1) % 8) for j in range(8)])

    def down_ring(a):
        return lax.ppermute(a, "y", [(j, (j - 1) % 8) for j in range(8)])

    def to_pair(a):
        return lax.ppermute(a, ("c", "zl"), [(3, 2)])

    line = line_up([lax.ppermute(packed, ("c", "x", "zl"), moves(d)) for d in (0, 1, -1, 2)])
    up_1 = up_ring(line)
    down_1 = down_ring(line)
    beside = (core_swap(gain), to_pair(images))
    up_2 = up_ring(up_1)
    early = line_up([line, up_1])
    down_1, early = lax.optimization_barrier((down_1, early))
    down_2 = down_ring(down_1)
    ordered = in_order(beside[1], images, gain, beside[0])
    up_2, ordered = lax.optimization_barrier((up_2, ordered))
    up_3 = up_ring(up_2)
    early = line_up([early, down_1, up_2])
    down_2, early = lax.optimization_barrier((down_2, early))
    down_3 = down_ring(down_2)
    first = line_up([early, down_2])
    other_first = core_swap(first)
    up_3, other_first = lax.optimization_barrier((up_3, other_first))
    up_4 = up_ring(half_of(up_3, 0))
    down_4 = down_ring(half_of(down_3, 1))
    second = line_up([up_3, down_3])
    other_second = core_swap(second)
    up_4, other_second = lax.optimization_barrier((up_4, other_second))
    third = line_up([up_4, down_4])
    other_third = core_swap(third)
    places = ((0, False), (320, False), (448, False), (0, True), (320, True))
    base = assemble(None, places, (first, second, third, other_first, other_second))
    return assemble(base, ((448, True),), (other_third,)), ordered


def rows_body(*refs):
    order, streams, out, rows = refs[0], refs[1:-2], refs[-2], refs[-1]
    rows[...] = jnp.zeros_like(rows)
    for i, stream in enumerate(streams):
        rows[i : i + 1] = stream[0:1].astype(jnp.float32)
    out[...] = dot_t(rows[...].astype(jnp.bfloat16), order[...]).astype(jnp.bfloat16)


def class_rows(order, streams):
    width = streams[0].shape[1]
    return pl.pallas_call(
        rows_body,
        out_shape=vmem((8, width)),
        in_specs=[VMEM_SPEC] * (1 + len(streams)),
        out_specs=VMEM_SPEC,
        scratch_shapes=[vmem((8, width), jnp.float32)],
        compiler_params=limit(),
        name="class_rows",
    )(order, *streams)


def sum_body(*refs):
    total = refs[0][...]
    for ref in refs[1:-1]:
        total = total + ref[...]
    refs[-1][...] = total


def one_of(parts):
    return pl.pallas_call(
        sum_body,
        out_shape=vmem(parts[0].shape),
        in_specs=[VMEM_SPEC] * len(parts),
        out_specs=VMEM_SPEC,
        compiler_params=limit(),
        name="one_of",
    )(*parts)


def final_body(mine, other, gain_ref, head_ref, mean_ref, variance_ref, normed):
    here = lax.axis_index("c") == lax.axis_index("zl")
    rows = jnp.where(here, mine[...], other[...]).astype(jnp.float32)
    streams = 1 + TANGENTS
    gain = gain_ref[...]
    normed[...] = jnp.zeros_like(normed)
    for image in range(mean_ref.shape[0]):
        at = image * streams
        x = rows[at : at + 1]
        c = x - row_mean(x)
        r = lax.rsqrt(row_mean(c * c) + epsilon)
        normed[at : at + 1] = c * r * gain
        for j in range(1, streams):
            t = rows[at + j : at + j + 1]
            dc = t - row_mean(t)
            dr = -(r * r * r) * row_mean(c * dc)
            normed[at + j : at + j + 1] = (dc * r + c * dr) * gain
    logits = dot(normed[...].astype(jnp.bfloat16), head_ref[...])
    for image in range(mean_ref.shape[0]):
        at = image * streams
        mean_ref[image] = logits[at : at + 1]
        tangents = [logits[at + j : at + j + 1] for j in range(1, streams)]
        variance_ref[image] = sum(t * t for t in tangents)


def final_logits(mine, other, gain, head, micro):
    shape = jax.ShapeDtypeStruct((micro, 1, head.shape[1]), jnp.float32)
    return pl.pallas_call(
        final_body,
        out_shape=(shape, shape),
        in_specs=[VMEM_SPEC] * 4,
        out_specs=(VMEM_SPEC,) * 2,
        scratch_shapes=[vmem(mine.shape, jnp.float32)],
        compiler_params=limit(),
        name="final_logits",
    )(mine, other, gain, head)


def cell(plane, core):
    return plane // 2 * 4 + core * 2 + plane % 2


def shards(tokens, w_qkv, w_output, tangent_value, tangent_output, layer_gain, final_gain, head):
    micro, _, length, width = tokens.shape
    images = tokens.reshape(micro, length, width)
    packed = pack(w_qkv, tangent_value, w_output, tangent_output)
    weights, (images, gain, order) = gathered(packed, layer_gain, images)

    stages = 8
    streams = (None,) * (1 + TANGENTS)
    last = []
    for step in range(stages + micro - 1):
        route = [
            (cell(s, c), cell(s + 1, 1 - c))
            for s in range(stages - 1)
            if 0 <= step - s < micro
            for c in range(2)
        ]
        out, normed, qkv, probs, attended = primal_layer(step, images, streams[0], gain, weights)
        results, moved = [out], []
        if route:
            moved.append(lax.ppermute(out, ("zh", "c", "zl"), route))
        saved = (qkv, probs, *shared_layer(step, weights, normed, attended))
        for which in range(TANGENTS):
            out = tangent_layer(
                which, step, images, streams[0], streams[1 + which], gain, weights, saved
            )
            results.append(out)
            if route:
                moved.append(lax.ppermute(out, ("zh", "c", "zl"), route))
        streams = tuple(moved)
        if step >= stages - 1:
            last += results
    rows = class_rows(order, last)
    sent = [
        lax.ppermute(
            rows,
            ("zh", "c", "zl"),
            [(cell(7, 1), cell(2 * i, 0)), (cell(7, 0), cell(2 * i + 1, 1))],
        )
        for i in range(4)
    ]
    mine = one_of(sent)
    return final_logits(mine, core_swap(mine), final_gain[None], head, micro)


def solution(mesh):
    sizes = (4, 2, 8, 4, 2)
    split = Mesh(mesh.devices.reshape(sizes), ("zh", "c", "y", "x", "zl"))
    section, dp = ("zh", "c"), ("y", "x", "zl")
    return jax.shard_map(
        shards,
        mesh=split,
        in_specs=(
            P(None, dp, None, None),
            P(section, dp, None),
            P(section, None, dp),
            P(section, None, dp, None),
            P(section, None, None, dp),
            P(section, None),
            P(),
            P(None, section),
        ),
        out_specs=(P(None, dp, section), P(None, dp, section)),
        check_vma=False,
    )
```

```python
import functools

import jax
import jax.numpy as jnp
from jax import lax
from jax.experimental import pallas as pl
from jax.experimental.pallas import tpu as pltpu
from jax.sharding import Mesh
from jax.sharding import PartitionSpec as P

HEADS = 8
HEAD = 64
TANGENTS = 2
HD = 512
PAIR = 2 * HEAD
PAIRS = HEADS // 2
SCALE = HEAD ** (-0.5)

epsilon = 1e-06
LAST_STEP = 8

QKV = slice(0, 3 * HD)
TV = (slice(3 * HD, 4 * HD), slice(4 * HD, 5 * HD))
WO = slice(5 * HD, 6 * HD)
TO = (slice(6 * HD, 7 * HD), slice(7 * HD, 8 * HD))


VMEM_SPEC = pl.BlockSpec(memory_space=pltpu.VMEM)
HBM_SPEC = pl.BlockSpec(memory_space=pltpu.HBM)


def dot(left, right):
    return jnp.dot(left, right, preferred_element_type=jnp.float32)


def dot_t(left, right):
    return lax.dot_general(
        left, right, (((1,), (1,)), ((), ())), preferred_element_type=jnp.float32
    )


def row_mean(a):
    return jnp.sum(a, -1, keepdims=True) * (1.0 / a.shape[-1])


def head_masks(rows):
    lane = lax.broadcasted_iota(jnp.int32, (rows, PAIR), 1)
    return lane < HEAD, lane >= HEAD


def part(ref, which, pair):
    at = which * HD + pair * PAIR
    return ref[:, at : at + PAIR]


def masked(a, mask):
    return jnp.where(mask, a, jnp.zeros_like(a))


def plane_of_this():
    return 2 * lax.axis_index("zh") + lax.axis_index("zl")


def wanted(step, tokens):
    return min(tokens, 16) if step == LAST_STEP else tokens


def working(step, plane):
    return (step - plane >= 0) & (step - plane < 2)


def entering(step, plane, images, stream, t_stream=None):
    if step < 2:
        x = images[step].astype(jnp.float32)
        t = jnp.zeros_like(x)
        if step == 1:
            x = jnp.where(plane == 0, x, stream[...].astype(jnp.float32))
            if t_stream is not None:
                t = jnp.where(plane == 0, t, t_stream[...].astype(jnp.float32))
        return x, t
    return (
        stream[...].astype(jnp.float32),
        None if t_stream is None else t_stream[...].astype(jnp.float32),
    )


def primal_body(step, *refs):
    gain_ref, w_ref, out_ref, n_ref, qkv_ref, p_ref, att_ref = refs[-7:]
    images, streams = refs[0] if step < 2 else None, refs[1 if step < 2 else 0 : -7]
    plane = plane_of_this()

    @pl.when(working(step, plane))
    def _():
        x, _ = entering(step, plane, images, *streams[:1] or (None,))
        gain = gain_ref[...]
        c = x - row_mean(x)
        r = lax.rsqrt(row_mean(c * c) + epsilon)
        n = (c * r * gain).astype(jnp.bfloat16)
        n_ref[...] = n
        qkv_ref[...] = dot(n, w_ref[:, QKV]).astype(jnp.bfloat16)
        masks = head_masks(x.shape[0])
        rows = wanted(step, x.shape[0])
        for pair in range(PAIRS):
            q, k, v = (part(qkv_ref, i, pair) for i in range(3))
            total = None
            for half in range(2):
                s = dot_t(masked(q, masks[half])[:rows], k) * SCALE
                e = jnp.exp(s - jnp.max(s, -1, keepdims=True))
                p = e / jnp.sum(e, -1, keepdims=True)
                p_ref[2 * pair + half, :rows] = p
                a = dot(p.astype(jnp.bfloat16), masked(v, masks[half]))
                total = a if total is None else total + a
            att_ref[:rows, pair * PAIR : (pair + 1) * PAIR] = total.astype(jnp.bfloat16)
        out_ref[:rows] = (x[:rows] + dot_t(att_ref[:rows], w_ref[:, WO])).astype(jnp.bfloat16)


def shared_body(step, w_ref, n_ref, att_ref, values_ref, outs_ref):
    @pl.when(working(step, plane_of_this()))
    def _():
        rows = wanted(step, att_ref.shape[0])
        for which in range(TANGENTS):
            values_ref[which] = dot(n_ref[...], w_ref[:, TV[which]])
            outs_ref[which, :rows] = dot_t(att_ref[:rows], w_ref[:, TO[which]])


def first_tangent(which, p_ref, values_ref, joined):
    masks = head_masks(joined.shape[0])
    for pair in range(PAIRS):
        at = slice(pair * PAIR, (pair + 1) * PAIR)
        v1 = values_ref[which, :, at].astype(jnp.bfloat16)
        total = None
        for half in range(2):
            a = dot(p_ref[2 * pair + half].astype(jnp.bfloat16), masked(v1, masks[half]))
            total = a if total is None else total + a
        joined[:, at] = total.astype(jnp.bfloat16)


def tangent_body(which, step, *refs):
    gain_ref, w_ref, qkv_ref, p_ref, values_ref, outs_ref, out_ref, mine, joined = refs[-9:]
    images, streams = refs[0] if step < 2 else None, refs[1 if step < 2 else 0 : -9]
    plane, rows = plane_of_this(), wanted(step, joined.shape[0])

    @pl.when(working(step, plane))
    def _():
        if step == 0:
            first_tangent(which, p_ref, values_ref, joined)
            t = jnp.zeros(out_ref.shape, jnp.float32)
        else:
            x, t = entering(step, plane, images, *streams)
            gain = gain_ref[...]
            c = x - row_mean(x)
            r = lax.rsqrt(row_mean(c * c) + epsilon)
            dc = t - row_mean(t)
            dr = -(r * r * r) * row_mean(c * dc)
            dn = ((dc * r + c * dr) * gain).astype(jnp.bfloat16)
            mine[:, : 2 * HD] = dot(dn, w_ref[:, : 2 * HD]).astype(jnp.bfloat16)
            values = dot(dn, w_ref[:, 2 * HD : 3 * HD]) + values_ref[which]
            mine[:, 2 * HD :] = values.astype(jnp.bfloat16)
            masks = head_masks(x.shape[0])
            for pair in range(PAIRS):
                q0, k0, v0 = (part(qkv_ref, i, pair) for i in range(3))
                q1, k1, v1 = (part(mine, i, pair) for i in range(3))
                total = None
                for half in range(2):
                    m = masks[half]
                    ds = (dot_t(masked(q1, m)[:rows], k0) + dot_t(masked(q0, m)[:rows], k1)) * SCALE
                    p = p_ref[2 * pair + half, :rows]
                    dp = p * (ds - jnp.sum(p * ds, -1, keepdims=True))
                    a = dot(dp.astype(jnp.bfloat16), masked(v0, m)) + dot(
                        p.astype(jnp.bfloat16), masked(v1, m)
                    )
                    total = a if total is None else total + a
                joined[:rows, pair * PAIR : (pair + 1) * PAIR] = total.astype(jnp.bfloat16)
        moved = dot_t(joined[:rows], w_ref[:, WO]) + outs_ref[which, :rows]
        out_ref[:rows] = (t[:rows] + moved).astype(jnp.bfloat16)


def cost(flops, bytes_accessed):
    return pl.CostEstimate(flops=flops, bytes_accessed=bytes_accessed, transcendentals=0)


def vmem(shape, dtype=jnp.bfloat16):
    return pltpu.VMEM(shape, dtype)


def in_hbm(a):
    return pltpu.with_memory_space_constraint(a, pltpu.HBM)


def limit(mib=4):
    return pltpu.CompilerParams(vmem_limit_bytes=mib << 20)


def primal_layer(step, images, x, gain, weights):
    tokens, width = images.shape[1:]
    bf16 = jnp.bfloat16
    given = (*((images,) if step < 2 else ()), *((x,) if step else ()), gain, weights)
    return pl.pallas_call(
        functools.partial(primal_body, step),
        out_shape=(
            jax.ShapeDtypeStruct((tokens, width), bf16),
            jax.ShapeDtypeStruct((tokens, width), bf16),
            jax.ShapeDtypeStruct((tokens, 3 * HD), bf16),
            jax.ShapeDtypeStruct((HEADS, tokens, tokens), jnp.float32),
            jax.ShapeDtypeStruct((tokens, HD), bf16),
        ),
        in_specs=[VMEM_SPEC] * len(given),
        out_specs=(VMEM_SPEC,) * 5,
        cost_estimate=cost(2 * tokens * width * 4 * HD, 1 << 20),
        compiler_params=limit(12),
        name="primal_layer",
    )(*given)


def shared_layer(step, weights, normed, attended):
    tokens, width = normed.shape
    return pl.pallas_call(
        functools.partial(shared_body, step),
        out_shape=(
            jax.ShapeDtypeStruct((TANGENTS, tokens, HD), jnp.float32),
            jax.ShapeDtypeStruct((TANGENTS, tokens, width), jnp.float32),
        ),
        in_specs=[VMEM_SPEC] * 3,
        out_specs=(VMEM_SPEC,) * 2,
        cost_estimate=cost(2 * tokens * width * 4 * HD, 1 << 20),
        compiler_params=limit(12),
        name="shared_layer",
    )(weights, normed, attended)


def tangent_layer(which, step, images, x, t, gain, weights, saved):
    tokens, width = images.shape[1:]
    given = (*((images,) if step < 2 else ()), *((x, t) if step else ()), gain, weights, *saved)
    return pl.pallas_call(
        functools.partial(tangent_body, which, step),
        out_shape=jax.ShapeDtypeStruct((tokens, width), jnp.bfloat16),
        in_specs=[VMEM_SPEC] * len(given),
        out_specs=VMEM_SPEC,
        scratch_shapes=[vmem((tokens, 3 * HD)), vmem((tokens, HD))],
        cost_estimate=cost(2 * tokens * width * 4 * HD, 1 << 20),
        compiler_params=limit(12),
    )(*given)


def copied(pairs, sems):
    copies = [pltpu.make_async_copy(a, b, sems.at[i]) for i, (a, b) in enumerate(pairs)]
    for copy in copies:
        copy.start()
    for copy in copies:
        copy.wait()


def pack_body(qkv, value, output, tangent_output, out, sems):
    pairs = [(qkv.at[0], out.at[:, QKV]), (output.at[0], out.at[:, WO])]
    for which in range(TANGENTS):
        pairs.append((value.at[0, which], out.at[:, TV[which]]))
        pairs.append((tangent_output.at[0, which], out.at[:, TO[which]]))
    copied(pairs, sems)


def pack(w_qkv, tangent_value, w_output, tangent_output):
    shares = (w_qkv, tangent_value, w_output.swapaxes(1, 2), tangent_output.swapaxes(2, 3))
    return pl.pallas_call(
        pack_body,
        out_shape=vmem((w_qkv.shape[1], 8 * HD)),
        in_specs=[HBM_SPEC] * 4,
        out_specs=VMEM_SPEC,
        scratch_shapes=[pltpu.SemaphoreType.DMA((2 + 2 * TANGENTS,))],
        compiler_params=limit(),
        name="pack",
    )(*map(in_hbm, shares))


def line_body(*refs):
    parts, out = refs[:-1], refs[-1]
    at = 0
    for part in parts:
        out[at : at + part.shape[0]] = part[...]
        at += part.shape[0]


def line_up(parts):
    rows, columns = sum(p.shape[0] for p in parts), parts[0].shape[1]
    return pl.pallas_call(
        line_body,
        out_shape=vmem((rows, columns)),
        in_specs=[VMEM_SPEC] * len(parts),
        out_specs=VMEM_SPEC,
        compiler_params=limit(),
        name="line_up",
    )(*parts)


def half_body(first, whole, out):
    out[...] = whole[first : first + out.shape[0]]


def half_of(whole, upper):
    rows, columns = whole.shape
    return pl.pallas_call(
        functools.partial(half_body, upper * (rows // 2)),
        out_shape=vmem((rows // 2, columns)),
        in_specs=[VMEM_SPEC],
        out_specs=VMEM_SPEC,
        compiler_params=limit(),
        name="half_of",
    )(whole)


def order_body(tokens, own_tokens, own_gain, other_gain, images_out, gain_out, order_out):
    core, y, x = lax.axis_index("c"), lax.axis_index("y"), lax.axis_index("x")
    width = order_out.shape[0]
    place = lax.broadcasted_iota(jnp.int32, (1, width), 1)
    half, row = place // (width // 2), place % (width // 2)
    piece, share, element = row // 64, row % 64 // 16, row % 16
    rise = jnp.where(piece % 2 == 1, -((piece + 1) // 2), piece // 2)
    along = jnp.where(share <= 1, -share, share - 1)
    at = ((y + rise + 8) % 8 * 4 + (x + along + 4) % 4) * 2 + (core + half) % 2
    feature = at * 16 + element
    one_hot = lax.broadcasted_iota(jnp.int32, (width, width), 0) == feature
    order_out[...] = one_hot.astype(jnp.float32).astype(jnp.bfloat16)
    order = order_out[...]
    for i in range(images_out.shape[0]):
        mine = jnp.where(core == 0, own_tokens[i], tokens[i])
        images_out[i] = dot(mine, order).astype(jnp.bfloat16)
    rest = jnp.where(core == lax.axis_index("zl"), own_gain[...], other_gain[...])
    gain = jnp.zeros_like(rest)
    for _ in range(3):
        high = rest.astype(jnp.bfloat16)
        rest = rest - high.astype(jnp.float32)
        gain = gain + dot(jnp.broadcast_to(high, (8, width)), order)[:1]
    gain_out[...] = gain


def in_order(tokens, own_tokens, own_gain, other_gain):
    width = tokens.shape[-1]
    return pl.pallas_call(
        order_body,
        out_shape=(vmem(tokens.shape), vmem(own_gain.shape, jnp.float32), vmem((width, width))),
        in_specs=[VMEM_SPEC] * 4,
        out_specs=(VMEM_SPEC,) * 3,
        compiler_params=limit(12),
        cost_estimate=cost(1 << 26, 1 << 20),
        name="in_order",
    )(tokens, own_tokens, own_gain, other_gain)


def assemble_body(first, aliased, *refs):
    pieces, out = refs[int(aliased) : -1], refs[-1]
    for at, piece in zip(first, pieces, strict=True):
        out[at : at + piece.shape[0]] = piece[...]


def assemble(base, first, pieces):
    columns = pieces[0].shape[1]
    given = [] if base is None else [base]
    return pl.pallas_call(
        functools.partial(assemble_body, first, base is not None),
        out_shape=vmem((1024, columns)),
        in_specs=[VMEM_SPEC] * (len(given) + len(pieces)),
        out_specs=VMEM_SPEC,
        input_output_aliases={0: 0} if given else {},
        cost_estimate=cost(1 << 24, 1 << 20),
        compiler_params=limit(),
        name="assemble",
    )(*given, *pieces)


def core_swap(a):
    return lax.ppermute(a, "c", [(0, 1), (1, 0)])


def gathered(packed, gain, images):
    def moves(d):
        cells = [(c, x, z) for c in range(2) for x in range(4) for z in range(2)]
        return [(8 * c + 2 * x + z, 8 * z + 2 * ((x + d) % 4) + c) for c, x, z in cells]

    def up_ring(a):
        return lax.ppermute(a, "y", [(j, (j + 1) % 8) for j in range(8)])

    def down_ring(a):
        return lax.ppermute(a, "y", [(j, (j - 1) % 8) for j in range(8)])

    def to_pair(a):
        return lax.ppermute(a, ("c", "zl"), [(3, 2)])

    line = line_up([lax.ppermute(packed, ("c", "x", "zl"), moves(d)) for d in (0, 1, -1, 2)])
    up_1 = up_ring(line)
    down_1 = down_ring(line)
    beside = (core_swap(gain), to_pair(images))
    up_2 = up_ring(up_1)
    early = line_up([line, up_1])
    down_1, early = lax.optimization_barrier((down_1, early))
    down_2 = down_ring(down_1)
    ordered = in_order(beside[1], images, gain, beside[0])
    up_2, ordered = lax.optimization_barrier((up_2, ordered))
    up_3 = up_ring(up_2)
    early = line_up([early, down_1, up_2])
    down_2, early = lax.optimization_barrier((down_2, early))
    down_3 = down_ring(down_2)
    first = line_up([early, down_2])
    other_first = core_swap(first)
    up_3, other_first = lax.optimization_barrier((up_3, other_first))
    up_4 = up_ring(half_of(up_3, 0))
    down_4 = down_ring(half_of(down_3, 1))
    second = line_up([up_3, down_3])
    other_second = core_swap(second)
    up_4, other_second = lax.optimization_barrier((up_4, other_second))
    third = line_up([up_4, down_4])
    other_third = core_swap(third)
    base = assemble(None, (0, 320, 448, 512, 832), (first, second, third, other_first, other_second))
    return assemble(base, (960,), (other_third,)), ordered


def rows_body(*refs):
    order, streams, out, rows = refs[0], refs[1:-2], refs[-2], refs[-1]
    rows[...] = jnp.zeros_like(rows)
    for i, stream in enumerate(streams):
        rows[i : i + 1] = stream[0:1].astype(jnp.float32)
    out[...] = dot_t(rows[...].astype(jnp.bfloat16), order[...]).astype(jnp.bfloat16)


def class_rows(order, streams):
    width = streams[0].shape[1]
    return pl.pallas_call(
        rows_body,
        out_shape=vmem((8, width)),
        in_specs=[VMEM_SPEC] * (1 + len(streams)),
        out_specs=VMEM_SPEC,
        scratch_shapes=[vmem((8, width), jnp.float32)],
        compiler_params=limit(),
        name="class_rows",
    )(order, *streams)


def sum_body(*refs):
    total = refs[0][...]
    for ref in refs[1:-1]:
        total = total + ref[...]
    refs[-1][...] = total


def one_of(parts):
    return pl.pallas_call(
        sum_body,
        out_shape=vmem(parts[0].shape),
        in_specs=[VMEM_SPEC] * len(parts),
        out_specs=VMEM_SPEC,
        compiler_params=limit(),
        name="one_of",
    )(*parts)


def final_body(mine, other, gain_ref, head_ref, mean_ref, variance_ref, normed):
    here = lax.axis_index("c") == lax.axis_index("zl")
    rows = jnp.where(here, mine[...], other[...]).astype(jnp.float32)
    streams = 1 + TANGENTS
    gain = gain_ref[...]
    normed[...] = jnp.zeros_like(normed)
    for image in range(mean_ref.shape[0]):
        at = image * streams
        x = rows[at : at + 1]
        c = x - row_mean(x)
        r = lax.rsqrt(row_mean(c * c) + epsilon)
        normed[at : at + 1] = c * r * gain
        for j in range(1, streams):
            t = rows[at + j : at + j + 1]
            dc = t - row_mean(t)
            dr = -(r * r * r) * row_mean(c * dc)
            normed[at + j : at + j + 1] = (dc * r + c * dr) * gain
    logits = dot(normed[...].astype(jnp.bfloat16), head_ref[...])
    for image in range(mean_ref.shape[0]):
        at = image * streams
        mean_ref[image] = logits[at : at + 1]
        tangents = [logits[at + j : at + j + 1] for j in range(1, streams)]
        variance_ref[image] = sum(t * t for t in tangents)


def final_logits(mine, other, gain, head, micro):
    shape = jax.ShapeDtypeStruct((micro, 1, head.shape[1]), jnp.float32)
    return pl.pallas_call(
        final_body,
        out_shape=(shape, shape),
        in_specs=[VMEM_SPEC] * 4,
        out_specs=(VMEM_SPEC,) * 2,
        scratch_shapes=[vmem(mine.shape, jnp.float32)],
        compiler_params=limit(),
        name="final_logits",
    )(mine, other, gain, head)


def shards(tokens, w_qkv, w_output, tangent_value, tangent_output, layer_gain, final_gain, head):
    micro, _, length, width = tokens.shape
    images = tokens.reshape(micro, length, width)
    packed = pack(w_qkv, tangent_value, w_output, tangent_output)
    weights, (images, gain, order) = gathered(packed, layer_gain, images)

    stages = 8
    streams = (None,) * (1 + TANGENTS)
    last = []
    for step in range(stages + micro - 1):
        route = [(s, s + 1) for s in range(stages - 1) if 0 <= step - s < micro]
        out, normed, qkv, probs, attended = primal_layer(step, images, streams[0], gain, weights)
        results, moved = [out], []
        if route:
            moved.append(lax.ppermute(out, ("zh", "zl"), route))
        saved = (qkv, probs, *shared_layer(step, weights, normed, attended))
        for which in range(TANGENTS):
            out = tangent_layer(
                which, step, images, streams[0], streams[1 + which], gain, weights, saved
            )
            results.append(out)
            if route:
                moved.append(lax.ppermute(out, ("zh", "zl"), route))
        streams = tuple(moved)
        if step >= stages - 1:
            last += results
    rows = class_rows(order, last)
    sent = [
        lax.ppermute(rows, ("zh", "c", "zl"), [(13, 4 * i), (15, 4 * i + 3)]) for i in range(4)
    ]
    mine = one_of(sent)
    return final_logits(mine, core_swap(mine), final_gain[None], head, micro)


def solution(mesh):
    sizes = (4, 2, 8, 4, 2)
    split = Mesh(mesh.devices.reshape(sizes), ("zh", "c", "y", "x", "zl"))
    section, dp = ("zh", "c"), ("y", "x", "zl")
    return jax.shard_map(
        shards,
        mesh=split,
        in_specs=(
            P(None, dp, None, None),
            P(section, dp, None),
            P(section, None, dp),
            P(section, None, dp, None),
            P(section, None, None, dp),
            P(section, None),
            P(),
            P(None, section),
        ),
        out_specs=(P(None, dp, section), P(None, dp, section)),
        check_vma=False,
    )
```
